512 devices in a mesh: grp: 4 (over y), row: 128 (over x, z, core).
Axes of the slice: x: 4, y: 4, z: 16, core: 2. Of those that a mesh axis runs over, the one named last changes fastest.
Arguments:
- a_tiles: bfloat16 [1024, 4, 7, 128, 128], P('row', 'grp'), may hold values from -0.5 to 0.5
- a_cols: int32 [1024, 4, 7], P('row', 'grp'), may hold values from 0 to 1023, as said below
- p_tiles: bfloat16 [1024, 4, 128, 128], P('row'), may hold values from -0.5 to 0.5
- p_cols: int32 [1024, 4], replicated, may hold values from 0 to 511, as said below
- c_cols: int32 [512, 16], replicated, may hold values from 0 to 511, as said below
Outputs:
- coarse: float32 [512, 16, 128, 128], P('row', 'grp')
The draws below stay inside these ranges and needn't reach their ends.
Inputs may be any that keep to these rules, and one draw needn't show every extreme that they name: For fine tile row i in block b = i // 8, every entry of a_cols[i] lies in [max(b - 2, 0) * 8, min(b + 3, 128) * 8). For fine tile row i in block b = i // 8, the entries of p_cols[i] are distinct and lie in [(b - 1) * 4, (b + 2) * 4). For coarse tile row c in block t = c // 4, the entries of c_cols[c] are distinct and lie among the 20 coarse tile rows that start at min(max(t - 2, 0), 123) * 4.
All inputs are finite; a program needn't handle non-finite values.
Results may differ from the reference program's by a relative error of at most 0.0003.
Values may be sent and summed in bfloat16 or wider, within the bound.
No kernel may reach another device: no remote copies, remote signals or barrier semaphores. Data moves between devices by JAX's collectives and lax.ppermute only.
A program may use at most 128 MiB of HBM per device.

```python
import jax
import jax.numpy as jnp
from jax import lax

TILE = 128
CT_DEV = 4
SLOTS = 7
KP = 4
KC = 16
FT_DEV = 8
GROUPS = 4
FT = 1024
NCT = 512


def pick_distinct(key, count, width, valid, take):
    offsets = jnp.arange(width, dtype=jnp.int32)[None, :]
    scores = jax.random.randint(key, (count, width), 0, 1 << 20, dtype=jnp.int32) * width + offsets
    scores = jnp.where(valid, scores, -1 - offsets)
    top_scores, chosen = lax.top_k(scores, take)
    return chosen.astype(jnp.int32)


def draw_a_cols(key, part):
    fine_ids = jnp.arange(FT, dtype=jnp.int32)
    owner = fine_ids // FT_DEV
    lowest = jnp.maximum(owner - 2, 0) * FT_DEV
    highest_row = jnp.minimum(owner + 3, FT // FT_DEV) * FT_DEV
    spans = (highest_row - lowest)[:, None, None]
    picks = jax.random.randint(jax.random.fold_in(key, 17), (FT, GROUPS, SLOTS), 0, 1 << 30, dtype=jnp.int32)
    return (lowest[:, None, None] + picks % spans).astype(jnp.int32)


def draw_p_cols(key, part):
    fine_ids = jnp.arange(FT, dtype=jnp.int32)
    owner = fine_ids // FT_DEV
    begin = (owner - 1) * CT_DEV
    candidate = begin[:, None] + jnp.arange(3 * CT_DEV, dtype=jnp.int32)[None, :]
    valid = (candidate >= 0) & (candidate < NCT)
    chosen = pick_distinct(jax.random.fold_in(key, 29), FT, 3 * CT_DEV, valid, KP)
    return (begin[:, None] + chosen).astype(jnp.int32)


def draw_c_cols(key, part):
    coarse_ids = jnp.arange(NCT, dtype=jnp.int32)
    owner = coarse_ids // CT_DEV
    begin = jnp.clip(owner - 2, 0, NCT // CT_DEV - 5) * CT_DEV
    valid = jnp.ones((NCT, 5 * CT_DEV), dtype=bool)
    chosen = pick_distinct(jax.random.fold_in(key, 41), NCT, 5 * CT_DEV, valid, KC)
    return (begin[:, None] + chosen).astype(jnp.int32)


def block_levels(own_key, dims, pieces, least, high):
    gain = 1.0
    for axis_at, blocks in pieces:
        draws = jax.random.uniform(jax.random.fold_in(jax.random.fold_in(own_key, 6), axis_at), (blocks,), jnp.float32, least / len(pieces), high / len(pieces))
        gain = gain * jnp.repeat(jnp.exp(draws), dims[axis_at] // blocks).reshape((-1,) + (1,) * (len(dims) - 1 - axis_at))
    return gain


def normal_values(rng, dims, scale, bound, split=(), kind=jnp.bfloat16):
    loudness = block_levels(rng, dims, split, -0.22, 0.18) if split else 1.0
    entries = jax.random.normal(rng, dims, jnp.float32) * scale * loudness
    return jnp.minimum(jnp.maximum(entries, -bound), bound).astype(kind)


def setup_inputs(seed: int = 0) -> dict:
    splits = jax.random.split(jax.random.key(seed), 6)
    a_tiles = normal_values(splits[0], (FT, GROUPS, SLOTS, TILE, TILE), TILE ** -0.5, 0.5, ((0, 128), (1, 4)))
    a_cols = draw_a_cols(jax.random.fold_in(splits[5], 71), 0)
    p_tiles = normal_values(splits[2], (FT, KP, TILE, TILE), TILE ** -0.5, 0.5, ((0, 128),))
    p_cols = draw_p_cols(jax.random.fold_in(splits[5], 71), 0)
    c_cols = draw_c_cols(jax.random.fold_in(splits[5], 71), 0)
    return dict(a_tiles=a_tiles, a_cols=a_cols, p_tiles=p_tiles, p_cols=p_cols, c_cols=c_cols)


highest = lax.Precision.HIGHEST


def reference(a_tiles, a_cols, p_tiles, p_cols, c_cols):
    def fine_row(coarse, inputs):
        a_row, columns, own_tiles, own_cols = inputs
        targets = c_cols[own_cols]
        fetched = p_tiles[columns].astype(jnp.float32)
        fetched_cols = p_cols[columns]
        products = jnp.einsum("gsxy,gspyz->gspxz", a_row.astype(jnp.float32), fetched, precision=highest)
        matches = (fetched_cols[:, :, :, None, None] == targets[None, None, None, :, :]).astype(jnp.float32)
        partial_value = jnp.einsum("gspxz,gspqk->gqkxz", products, matches, precision=highest)
        summed = jnp.sum(partial_value, axis=0)
        row_terms = jnp.einsum("qyx,qkyz->qkxz", own_tiles.astype(jnp.float32), summed, precision=highest)
        return coarse.at[own_cols].add(row_terms), None

    initial = jnp.zeros((NCT, KC, TILE, TILE), jnp.float32)
    result = lax.scan(fine_row, initial, (a_tiles, a_cols, p_tiles, p_cols))[0]
    return result
```

```python
import functools

import jax
import jax.numpy as jnp
from jax import lax
from jax.experimental import pallas as pl
from jax.experimental.pallas import tpu as pltpu
from jax.sharding import PartitionSpec as P


T = 128
F = 8
C = 4
S = 7
KP = 4
KC = 16
G = 4
KG = KC // G
NW = 7 * C
HC = 2
ROWS = HC * KG * T
SCALES = 16
PACK = ROWS + SCALES
LEVELS = 32760.0


def code(x, scratch, row):
    top = jnp.maximum(jnp.max(jnp.abs(x), axis=0, keepdims=True), 1e-37)
    exponent = jnp.floor(jnp.log2(top)) + 1.0
    scratch[pl.ds(row, 1), :] = exponent
    return jnp.round(x * (jnp.exp2(-exponent) * LEVELS)).astype(jnp.int32).astype(jnp.int16)


def widen(x):
    return x.astype(jnp.int32).astype(jnp.float32)


def products_kernel(
    part, pidx, wcol, first, lrow, sidx, odd, a_hbm, l_hbm, o_hbm, r_hbm, x_hbm, y_hbm, pt_hbm,
    *refs,
):
    if part == "outer":
        out0, out1, a_v, p_v, pt_v, acc, sp, tot, ex, sem = refs
    else:
        inner, own, a_v, p_v, pt_v, acc, sp, tot, ex, sem = refs
    copies = [pltpu.make_async_copy(a_hbm, a_v, sem.at[0])]
    for n, ref in enumerate((l_hbm, o_hbm, r_hbm, x_hbm, y_hbm)):
        copies.append(pltpu.make_async_copy(ref, p_v.at[n], sem.at[n + 1]))
    copies.append(pltpu.make_async_copy(pt_hbm, pt_v, sem.at[6]))
    for c in copies:
        c.start()
    nc = C if part == "outer" else 2 * C
    if part == "outer":
        base = odd[0] * (2 * C)
    else:
        base = (1 - odd[0]) * C

    def zero(c, _):
        tot[c] = jnp.zeros((KC, T, T), jnp.float32)
        return 0

    lax.fori_loop(0, nc, zero, 0)
    sp[NW] = jnp.zeros((2 * T, T), jnp.bfloat16)
    for c in copies:
        c.wait()

    def row(i, _):
        for s in range(S):
            a = a_v[i, s]
            j = pidx[i, s]
            blk, r = j // F, j % F
            for h in range(KP // 2):
                rhs = jnp.concatenate([p_v[blk, r, 2 * h], p_v[blk, r, 2 * h + 1]], axis=1)
                prod = jnp.dot(a, rhs, preferred_element_type=jnp.float32)
                for e in range(2):
                    m = s * KP + 2 * h + e
                    w = wcol[i, m]
                    old = jnp.where(first[i, m] == 1, 0.0, acc[w])
                    acc[w] = old + prod[:, e * T : (e + 1) * T]

        def split(w, _):
            x = acc[w]
            hi = x.astype(jnp.bfloat16)
            sp[w, 0:T, :] = hi
            sp[w, T : 2 * T, :] = (x - hi.astype(jnp.float32)).astype(jnp.bfloat16)
            return 0

        lax.fori_loop(0, NW, split, 0, unroll=4)
        for q in range(KP):
            c = lrow[i, q] - base

            @pl.when((c >= 0) & (c < nc))
            def _():
                pt = pt_v[i, q]
                lhs = jnp.concatenate([pt, pt], axis=1)
                for kk in range(KC // 2):
                    s0 = sidx[i * KP + q, 2 * kk]
                    s1 = sidx[i * KP + q, 2 * kk + 1]
                    rhs = jnp.concatenate([sp[s0], sp[s1]], axis=1)
                    prod = jnp.dot(lhs, rhs, preferred_element_type=jnp.float32)
                    tot[c, 2 * kk] += prod[:, :T]
                    tot[c, 2 * kk + 1] += prod[:, T:]

        return 0

    lax.fori_loop(0, F, row, 0)

    if part == "outer":
        start = 0
        dests = (out0, out1)
    else:
        start = odd[0] * 0 + (1 - odd[0]) * C
        dests = (inner.at[0], inner.at[1])
    for h in range(2):
        def group(g, _):
            for c in range(HC):
                for k in range(KG):
                    t = c * KG + k
                    dests[h][g, t * T : (t + 1) * T, :] = code(
                        tot[start + h * HC + c, g * KG + k], ex, t
                    )
            dests[h][g, ROWS:PACK, :] = ex[...].astype(jnp.int32).astype(jnp.int16)
            return 0

        lax.fori_loop(0, G, group, 0)
    if part == "rest":
        mine = odd[0] * C
        for c in range(C):
            own[c] = tot[mine + c]


def sum_kernel(own, inner, outer, out, ex_i, ex_o, ex):
    ex_i[...] = jnp.exp2(widen(inner[0, 0, ROWS:PACK, :])) * (1.0 / LEVELS)
    ex_o[...] = jnp.exp2(widen(outer[0, ROWS:PACK, :])) * (1.0 / LEVELS)
    for c in range(HC):
        for k in range(KG):
            t = c * KG + k
            rows = slice(t * T, (t + 1) * T)
            x = own[c, k] + widen(inner[0, 0, rows, :]) * ex_i[t : t + 1, :]
            x = x + widen(outer[0, rows, :]) * ex_o[t : t + 1, :]
            out[0, rows, :] = code(x, ex, t)
    out[0, ROWS:PACK, :] = ex[...].astype(jnp.int32).astype(jnp.int16)


def final_kernel(r0, r1, out, ex):
    for h, r in enumerate((r0, r1)):
        for g in range(G):
            ex[g] = jnp.exp2(widen(r[g, ROWS:PACK, :])) * (1.0 / LEVELS)
        for c in range(HC):
            for k in range(KG):
                t = c * KG + k
                rows = slice(t * T, (t + 1) * T)
                x = widen(r[0, rows, :]) * ex[0, t : t + 1, :]
                for g in range(1, G):
                    x = x + widen(r[g, rows, :]) * ex[g, t : t + 1, :]
                out[h * HC + c, k] = x


def permuted(x, to):
    n = lax.axis_size("row")
    return lax.ppermute(x, "row", [(i, to(i) % n) for i in range(n)])


def tables(a_cols, p_cols, c_cols, b):
    j = a_cols[:, 0, :]
    odd = b % 2
    rel = j // F - b
    near = 1 - 2 * odd
    slot = jnp.where(rel == -2, 0, jnp.where(rel == 0, 1, jnp.where(rel == 2, 2, jnp.where(rel == near, 3, 4))))
    pidx = slot * F + j % F
    wcol = p_cols[j].reshape(F, S * KP) - (b - 3) * C
    m = jnp.arange(S * KP, dtype=jnp.int32)
    same = wcol[:, :, None] == wcol[:, None, :]
    first = 1 - jnp.any(same & (m[None, None, :] < m[None, :, None]), axis=2).astype(jnp.int32)
    own = lax.dynamic_slice_in_dim(p_cols, b * F, F, 0)
    lrow = own - (b - 1) * C
    want = c_cols[own] - (b - 3) * C
    filled = jnp.any(want[..., None] == wcol[:, None, None, :], axis=-1)
    sidx = jnp.where(filled, want, NW).reshape(F * KP, KC)
    return pidx, wcol, first, lrow, sidx, jnp.full((1,), odd, jnp.int32)


def products(part, tabs, arrays):
    smem = pl.BlockSpec(memory_space=pltpu.SMEM)
    anyspace = pl.BlockSpec(memory_space=pl.ANY)
    vmem = pl.BlockSpec(memory_space=pltpu.VMEM)
    if part == "outer":
        out_shape = [jax.ShapeDtypeStruct((G, PACK, T), jnp.int16)] * 2
        nc = C
    else:
        out_shape = [
            jax.ShapeDtypeStruct((2, G, PACK, T), jnp.int16),
            jax.ShapeDtypeStruct((C, KC, T, T), jnp.float32),
        ]
        nc = 2 * C
    return pl.pallas_call(
        functools.partial(products_kernel, part),
        out_shape=out_shape,
        in_specs=[smem] * 6 + [anyspace] * 7,
        out_specs=[vmem] * 2,
        scratch_shapes=[
            pltpu.VMEM((F, S, T, T), jnp.bfloat16),
            pltpu.VMEM((5, F, KP, T, T), jnp.bfloat16),
            pltpu.VMEM((F, KP, T, T), jnp.bfloat16),
            pltpu.VMEM((NW, T, T), jnp.float32),
            pltpu.VMEM((NW + 1, 2 * T, T), jnp.bfloat16),
            pltpu.VMEM((nc, KC, T, T), jnp.float32),
            pltpu.VMEM((SCALES, T), jnp.float32),
            pltpu.SemaphoreType.DMA((7,)),
        ],
        compiler_params=pltpu.CompilerParams(vmem_limit_bytes=48 * 1024 * 1024),
        cost_estimate=pl.CostEstimate(flops=3 * 10**9, bytes_accessed=10**7, transcendentals=0),
    )(*tabs, *arrays)


def summed(h, own, inner, outer):
    return pl.pallas_call(
        sum_kernel,
        name="summed",
        out_shape=jax.ShapeDtypeStruct((G, PACK, T), jnp.int16),
        grid=(G,),
        in_specs=[
            pl.BlockSpec((HC, KG, T, T), lambda g: (h, g, 0, 0)),
            pl.BlockSpec((1, 1, PACK, T), lambda g: (h, g, 0, 0)),
            pl.BlockSpec((1, PACK, T), lambda g: (g, 0, 0)),
        ],
        out_specs=pl.BlockSpec((1, PACK, T), lambda g: (g, 0, 0)),
        scratch_shapes=[pltpu.VMEM((SCALES, T), jnp.float32)] * 3,
        cost_estimate=pl.CostEstimate(flops=10**8, bytes_accessed=5 * 10**6, transcendentals=0),
    )(own, inner, outer)


def finished(r0, r1):
    return pl.pallas_call(
        final_kernel,
        name="finished",
        out_shape=jax.ShapeDtypeStruct((C, KG, T, T), jnp.float32),
        scratch_shapes=[pltpu.VMEM((G, SCALES, T), jnp.float32)],
        cost_estimate=pl.CostEstimate(flops=10**8, bytes_accessed=4 * 10**6, transcendentals=0),
    )(r0, r1)


def body(a_tiles, a_cols, p_tiles, p_cols, c_cols):
    b = lax.axis_index("row")
    a = a_tiles[:, 0]
    right = permuted(p_tiles, lambda i: i - 2)
    left = permuted(p_tiles, lambda i: i + 2)
    near = permuted(p_tiles, lambda i: i ^ 1)
    tabs = tables(a_cols, p_cols, c_cols, b)
    pt = jnp.swapaxes(p_tiles, 2, 3)
    left, right, tabs, pt = lax.optimization_barrier((left, right, tabs, pt))
    far = permuted(jnp.where(b % 2 == 0, right, left), lambda i: i ^ 1)
    arrays = (a, left, p_tiles, right, near, far, pt)
    out0, out1 = products("outer", tabs, arrays)
    out0, out1, tabs = lax.optimization_barrier((out0, out1, tabs))
    away = lambda i: i - 1 if i % 2 == 0 else i + 1
    got0 = permuted(out0, away)
    got1 = permuted(out1, away)
    inner, own = products("rest", tabs, arrays)
    got = permuted(inner, lambda i: i ^ 1)
    results = []
    for h, outer in enumerate((got0, got1)):
        x = summed(h, own, got, outer)
        results.append(lax.all_to_all(x, "grp", 0, 0, tiled=True))
    return finished(*results)


def solution(mesh):
    return jax.shard_map(
        body,
        mesh=mesh,
        in_specs=(
            P("row", "grp", None, None, None),
            P("row", "grp", None),
            P("row", None, None, None),
            P(),
            P(),
        ),
        out_specs=P("row", "grp", None, None),
        check_vma=False,
    )
```

```python
import functools

import jax
import jax.numpy as jnp
from jax import lax
from jax.experimental import pallas as pl
from jax.experimental.pallas import tpu as pltpu
from jax.sharding import PartitionSpec as P


T = 128
F = 8
C = 4
S = 7
KP = 4
KC = 16
G = 4
KG = KC // G
N = S * KP
U = 4
NE = 72
SPARE = F * N
ZERO = SPARE + 1
NS = ZERO + 1
HC = 2
TC = HC * KG
ROWS = TC * T
SCALES = 16
PACK = ROWS + SCALES
LEVELS = 32760.0
MB = 1 << 20

SMEM = pl.BlockSpec(memory_space=pltpu.SMEM)
VMEM = pl.BlockSpec(memory_space=pltpu.VMEM)


def near_memory(x):
    return pltpu.with_memory_space_constraint(x, pltpu.VMEM)


def code(x, scratch, row):
    top = jnp.maximum(jnp.max(jnp.abs(x), axis=0, keepdims=True), 1e-37)
    exponent = jnp.floor(jnp.log2(top)) + 1.0
    scratch[pl.ds(row, 1), :] = exponent
    return jnp.round(x * (jnp.exp2(-exponent) * LEVELS)).astype(jnp.int32).astype(jnp.int16)


def widen(x):
    return x.astype(jnp.int32).astype(jnp.float32)


def params(mib):
    return pltpu.CompilerParams(vmem_limit_bytes=mib * MB)


def cost(flops):
    return pl.CostEstimate(flops=flops, bytes_accessed=10**6, transcendentals=0)


def tables(a_cols, p_cols, c_cols, b):
    i32 = jnp.int32
    j = a_cols.reshape(F * S)
    odd = b % 2
    rel = j // F - b
    near = 1 - 2 * odd
    seg = jnp.where(rel == 0, 0, jnp.where(rel == near, 1, jnp.where(rel == -2, 2, jnp.where(rel == 2, 3, 4))))
    e = jnp.arange(F * S, dtype=i32)
    same = seg[:, None] == seg[None, :]
    before = jnp.sum((same & (e[None, :] < e[:, None])).astype(i32), axis=1)
    count = jnp.sum((seg[None, :] == jnp.arange(5, dtype=i32)[:, None]).astype(i32), axis=1)
    steps = (count + U - 1) // U
    five = jnp.arange(6, dtype=i32)
    start = jnp.sum(jnp.where(five[None, :5] < five[:, None], steps[None, :], 0), axis=1)
    pos = jnp.sum(jnp.where(seg[:, None] == five[None, :5], start[None, :5], 0), axis=1) * U + before
    band0 = jnp.clip((b - 2) * F, 0, p_cols.shape[0] - 5 * F)
    band = lax.dynamic_slice_in_dim(p_cols, band0, 5 * F, 0)
    hit = (j - band0)[:, None] == jnp.arange(5 * F, dtype=i32)[None, :]
    wcol = jnp.sum(jnp.where(hit[:, :, None], band[None], 0), axis=1) - (b - 3) * C
    w = wcol.reshape(F, N)
    key = (pos[:, None] * KP + jnp.arange(KP, dtype=i32)[None, :]).reshape(F, N)
    dup = (w[:, :, None] == w[:, None, :]) & (key[:, None, :] < key[:, :, None])
    first = 1 - jnp.any(dup, axis=2).astype(i32)
    rank = jnp.sum(jnp.where(w[:, None, :] < w[:, :, None], first[:, None, :], 0), axis=2)
    many = jnp.sum(first, axis=1)
    rows = jnp.arange(F, dtype=i32)
    base = jnp.sum(jnp.where(rows[None, :] < rows[:, None], many[None, :], 0), axis=1)
    slot = (base[:, None] + rank).reshape(F * S, KP)
    place = pos[None, :] == jnp.arange(NE, dtype=i32)[:, None]
    taken = jnp.any(place, axis=1)

    def listed(x, empty):
        return jnp.where(taken[:, None], jnp.sum(jnp.where(place[:, :, None], x[None], 0), axis=1), empty)

    head = listed(jnp.stack([e, j % F], axis=1), 0)
    slots = listed(slot, SPARE)
    firsts = listed(first.reshape(F * S, KP), 1)
    entries = jnp.concatenate([head, slots, firsts], axis=1)

    own = lax.dynamic_slice_in_dim(p_cols, b * F, F, 0)
    row0 = jnp.clip((b - 1) * C, 0, c_cols.shape[0] - 3 * C)
    crows = lax.dynamic_slice_in_dim(c_cols, row0, 3 * C, 0)
    chit = (own.reshape(F * KP) - row0)[:, None] == jnp.arange(3 * C, dtype=i32)[None, :]
    want = jnp.sum(jnp.where(chit[:, :, None], crows[None], 0), axis=1) - (b - 3) * C
    want = want.reshape(F, KP * KC)
    filled = jnp.any(want[:, :, None] == w[:, None, :], axis=2)
    below = jnp.sum(jnp.where(w[:, None, :] < want[:, :, None], first[:, None, :], 0), axis=2)
    sidx = jnp.where(filled, base[:, None] + below, ZERO).reshape(F * KP, KC)

    local = own.reshape(F * KP) - (b - 1) * C
    left_first = local // C
    kind = jnp.where(left_first == 1, 2, jnp.where((left_first == 0) == (odd == 0), 0, 1))
    crow = kind * C + local % C
    pr = jnp.arange(F * KP, dtype=i32)
    ahead = (crow[None, :] < crow[:, None]) | ((crow[None, :] == crow[:, None]) & (pr[None, :] < pr[:, None]))
    ppos = jnp.sum(ahead.astype(i32), axis=1)
    cs = jnp.arange(16, dtype=i32)
    cstart = jnp.sum((crow[None, :] < cs[:, None]).astype(i32), axis=1)
    plist = jnp.sum(jnp.where(ppos[None, :] == pr[:, None], pr[None, :], 0), axis=1)
    small = jnp.concatenate([start, jnp.sum(many)[None], odd.reshape(1).astype(i32), cstart, plist])
    return entries, small, sidx


CSTART, PLIST, TOTAL, ODD = 8, 24, 6, 7


def entry_loop(seg, small, entries, a, p, acc):
    def step(t, _):
        for u in range(U):
            r = t * U + u
            j = entries[r, 1]
            rhs = jnp.concatenate([p[j, k] for k in range(KP)], axis=1)
            prod = jnp.dot(a[entries[r, 0]], rhs, preferred_element_type=jnp.float32)
            for k in range(KP):
                slot = entries[r, 2 + k]
                old = jnp.where(entries[r, 2 + KP + k] == 1, 0.0, acc[slot])
                acc[slot] = old + prod[:, k * T : (k + 1) * T]
        return 0

    lax.fori_loop(small[seg], small[seg + 1], step, 0)


def early_kernel(segs, small, entries, a, p0, p1, *refs):
    acc = refs[-1]
    entry_loop(segs[0], small, entries, a, p0, acc)
    entry_loop(segs[1], small, entries, a, p1, acc)


def last_kernel(small, entries, a, p, acc_in, acc, sp):
    entry_loop(4, small, entries, a, p, acc)
    sp[ZERO] = jnp.zeros((2 * T, T), jnp.bfloat16)

    def split(t, _):
        for u in range(4):
            n = t * 4 + u
            x = acc[n]
            hi = x.astype(jnp.bfloat16)
            sp[n, 0:T, :] = hi
            sp[n, T : 2 * T, :] = (x - hi.astype(jnp.float32)).astype(jnp.bfloat16)
        return 0

    lax.fori_loop(0, (small[TOTAL] + 3) // 4, split, 0)


ACC = pltpu.VMEM((NS, T, T), jnp.float32)


def early(segs, tabs, a, p0, p1, acc=None):
    entries, small, _ = tabs
    args = [small, entries, near_memory(a), near_memory(p0), near_memory(p1)]
    alias = {}
    if acc is not None:
        args.append(near_memory(acc))
        alias = {5: 0}
    return pl.pallas_call(
        functools.partial(early_kernel, segs),
        out_shape=ACC,
        in_specs=[SMEM] * 2 + [VMEM] * (len(args) - 2),
        out_specs=VMEM,
        input_output_aliases=alias,
        compiler_params=params(4),
        cost_estimate=cost(2 * 10**7),
    )(*args)


def last(tabs, a, p, acc):
    entries, small, _ = tabs
    return pl.pallas_call(
        last_kernel,
        name="last",
        out_shape=[ACC, pltpu.VMEM((NS, 2 * T, T), jnp.bfloat16)],
        in_specs=[SMEM] * 2 + [VMEM] * 3,
        out_specs=[VMEM] * 2,
        input_output_aliases={4: 0},
        compiler_params=params(4),
        cost_estimate=cost(2 * 10**7),
    )(small, entries, near_memory(a), near_memory(p), near_memory(acc))[1]


def coarse_kernel(rows, small, sidx, sp, pt, *refs):
    outs, ex = refs[:-1], refs[-1]

    def body(*accs):
        for acc in accs:
            pltpu.matmul_pop(acc)
        for c, (kind, dest, at, *half) in rows:
            out = outs[dest].at[half[0]] if half else outs[dest]
            e0 = half[0] * G * SCALES if half else 0

            def pair(r, _):
                pr = small[PLIST + r]
                tile = pt[pr]
                lhs = jnp.concatenate([tile, tile], axis=1)
                for n in range(KC // 2):
                    rhs = jnp.concatenate([sp[sidx[pr, 2 * n]], sp[sidx[pr, 2 * n + 1]]], axis=1)
                    pltpu.matmul_push_rhs(rhs, staging_register=(n // 2) % 2, mxu_index=n % 2)
                    pltpu.matmul_acc_lhs(accs[n], lhs, load_staged_rhs=(n // 2) % 2)
                return 0

            lax.fori_loop(small[CSTART + c], small[CSTART + c + 1], pair, 0)
            for n in range(KC // 2):
                x = pltpu.matmul_pop(accs[n])
                for h in range(2):
                    k = 2 * n + h
                    y = x[:, h * T : (h + 1) * T]
                    if kind == "plain":
                        out[at, k] = y
                    else:
                        g, t = k // KG, at * KG + k % KG
                        out[g, t * T : (t + 1) * T, :] = code(y, ex, e0 + g * SCALES + t)
            if kind == "code" and at == HC - 1:
                for g in range(G):
                    r0 = e0 + g * SCALES
                    out[g, ROWS:PACK, :] = ex[r0 : r0 + SCALES, :].astype(jnp.int32).astype(jnp.int16)

    pl.run_scoped(body, *[pltpu.ACC(n % 2)((T, 2 * T), jnp.float32) for n in range(KC // 2)])


def coarse(rows, out_shape, tabs, sp, pt):
    _, small, sidx = tabs
    return pl.pallas_call(
        functools.partial(coarse_kernel, rows),
        out_shape=out_shape,
        in_specs=[SMEM] * 2 + [VMEM] * 2,
        out_specs=[VMEM] * len(out_shape),
        scratch_shapes=[pltpu.VMEM((2 * G * SCALES, T), jnp.float32)],
        compiler_params=params(4),
        cost_estimate=cost(2 * 10**7),
    )(small, sidx, near_memory(sp), near_memory(pt))


CHUNK = pltpu.VMEM((G, PACK, T), jnp.int16)


def outer_chunk(h, tabs, sp, pt):
    rows = [(HC * h + c, ("code", 0, c)) for c in range(HC)]
    return coarse(rows, [CHUNK], tabs, sp, pt)[0]


def inner_chunks(tabs, sp, pt):
    rows = [(C + HC * h + c, ("code", 0, c, h)) for h in range(2) for c in range(HC)]
    shape = pltpu.VMEM((2, G, PACK, T), jnp.int16)
    return coarse(rows, [shape], tabs, sp, pt)[0]


def own_rows(tabs, sp, pt):
    rows = [(2 * C + c, ("plain", 0, c)) for c in range(C)]
    return coarse(rows, [pltpu.VMEM((C, KC, T, T), jnp.float32)], tabs, sp, pt)[0]


def pick_kernel(small, left, right, out):
    @pl.when(small[ODD] == 0)
    def _():
        out[...] = right[...]

    @pl.when(small[ODD] == 1)
    def _():
        out[...] = left[...]


def picked(tabs, left, right):
    return pl.pallas_call(
        pick_kernel,
        name="picked",
        out_shape=pltpu.VMEM(left.shape, left.dtype),
        in_specs=[SMEM] + [VMEM] * 2,
        out_specs=VMEM,
        compiler_params=params(4),
        cost_estimate=cost(10**6),
    )(tabs[1], near_memory(left), near_memory(right))


def sum_kernel(h, group, own, inner, outer, mine, *refs):
    sends, (ex_i, ex_o, ex) = refs[:3], refs[3:]
    for step in range(G):
        g = lax.rem(group[0] + step, G)
        ex_i[...] = jnp.exp2(widen(inner[h, g, ROWS:PACK, :])) * (1.0 / LEVELS)
        ex_o[...] = jnp.exp2(widen(outer[g, ROWS:PACK, :])) * (1.0 / LEVELS)
        for c in range(HC):
            for k in range(KG):
                t = c * KG + k
                rows = slice(t * T, (t + 1) * T)
                x = own[h * HC + c, g * KG + k] + widen(inner[h, g, rows, :]) * ex_i[t : t + 1, :]
                x = x + widen(outer[g, rows, :]) * ex_o[t : t + 1, :]
                if step == 0:
                    mine[c, k] = x
                else:
                    sends[step - 1][rows, :] = code(x, ex, t)
        if step:
            sends[step - 1][ROWS:PACK, :] = ex[...].astype(jnp.int32).astype(jnp.int16)


def summed(h, group, own, inner, outer):
    piece = pltpu.VMEM((PACK, T), jnp.int16)
    return pl.pallas_call(
        functools.partial(sum_kernel, h),
        out_shape=[pltpu.VMEM((HC, KG, T, T), jnp.float32)] + [piece] * 3,
        in_specs=[SMEM] + [VMEM] * 3,
        out_specs=[VMEM] * 4,
        scratch_shapes=[pltpu.VMEM((SCALES, T), jnp.float32)] * 3,
        compiler_params=params(4),
        cost_estimate=cost(10**7),
    )(group, near_memory(own), near_memory(inner), near_memory(outer))


def final_kernel(*refs):
    out, ex = refs[-2:]
    for h in range(2):
        mine, *got = refs[4 * h : 4 * h + 4]
        for n, r in enumerate(got):
            ex[n] = jnp.exp2(widen(r[ROWS:PACK, :])) * (1.0 / LEVELS)
        for c in range(HC):
            for k in range(KG):
                t = c * KG + k
                rows = slice(t * T, (t + 1) * T)
                x = mine[c, k]
                for n, r in enumerate(got):
                    x = x + widen(r[rows, :]) * ex[n, t : t + 1, :]
                out[h * HC + c, k] = x


def finished(parts):
    return pl.pallas_call(
        final_kernel,
        name="finished",
        out_shape=jax.ShapeDtypeStruct((C, KG, T, T), jnp.float32),
        in_specs=[VMEM] * 8,
        out_specs=VMEM,
        scratch_shapes=[pltpu.VMEM((G, SCALES, T), jnp.float32)],
        compiler_params=params(8),
        cost_estimate=cost(10**7),
    )(*[near_memory(x) for x in parts])


def permuted(x, axis, to):
    n = lax.axis_size(axis)
    return lax.ppermute(x, axis, [(i, to(i) % n) for i in range(n)])


def other(i):
    return i ^ 1


def away(i):
    return i - 1 if i % 2 == 0 else i + 1


def body(a_tiles, a_cols, p_tiles, p_cols, c_cols):
    b = lax.axis_index("row")
    group = lax.axis_index("grp").astype(jnp.int32).reshape(1)
    a = a_tiles.reshape(F * S, T, T)
    left = permuted(p_tiles, "row", lambda i: i + 2)
    right = permuted(p_tiles, "row", lambda i: i - 2)
    near = permuted(p_tiles, "row", other)
    tabs = tables(a_cols, p_cols, c_cols, b)
    pt = jnp.swapaxes(p_tiles, 2, 3).reshape(F * KP, T, T)
    tabs, pt, near, group = lax.optimization_barrier((tabs, pt, near, group))
    acc = early((0, 1), tabs, a, p_tiles, near)
    left, right, acc = lax.optimization_barrier((left, right, acc))
    far = permuted(picked(tabs, left, right), "row", other)
    acc = early((2, 3), tabs, a, left, right, acc)
    sp = last(tabs, a, far, acc)
    out0 = outer_chunk(0, tabs, sp, pt)
    got0 = permuted(out0, "row", away)
    out1 = outer_chunk(1, tabs, sp, pt)
    got1 = permuted(out1, "row", away)
    ins = inner_chunks(tabs, sp, pt)
    inner = permuted(ins, "row", other)
    own = own_rows(tabs, sp, pt)
    parts = []
    for h, outer in enumerate((got0, got1)):
        mine, *sends = summed(h, group, own, inner, outer)
        parts.append(mine)
        for n, x in enumerate(sends):
            parts.append(permuted(x, "grp", lambda i, n=n: i + n + 1))
    return finished(parts)


def solution(mesh):
    return jax.shard_map(
        body,
        mesh=mesh,
        in_specs=(
            P("row", "grp", None, None, None),
            P("row", "grp", None),
            P("row", None, None, None),
            P(),
            P(),
        ),
        out_specs=P("row", "grp", None, None),
        check_vma=False,
    )
```

```python
import functools

import jax
import jax.numpy as jnp
from jax import lax
from jax.experimental import pallas as pl
from jax.experimental.pallas import tpu as pltpu
from jax.sharding import PartitionSpec as P


T = 128
F = 8
C = 4
S = 7
KP = 4
KC = 16
G = 4
KG = KC // G
KD = 2 * KG
NA = F * S
HC = 2
TC = HC * KG
ROWS = TC * T
SCALES = 16
PACK = ROWS + SCALES
LEVELS = 32760.0
MB = 1 << 20

NW = 7 * C
SPARE = F * NW
ZERO = SPARE + 1
NS = ZERO + 1

LISTS = 5
U = 4
FRONT = U
CAP = FRONT + 2 * NA + 2 * U
WORDS = 1 + KP
PAIRS, PLIST = 0, 16
SMALL = PLIST + 3 * C * F * KP

SMEM = pl.BlockSpec(memory_space=pltpu.SMEM)
VMEM = pl.BlockSpec(memory_space=pltpu.VMEM)
HBM = pl.BlockSpec(memory_space=pltpu.HBM)


def call(kernel, args, outs, scratch=(), alias={}, mib=4):
    spec = {"smem": SMEM, "vmem": VMEM, "hbm": HBM}
    put = {
        "smem": lambda x: pltpu.with_memory_space_constraint(x, pltpu.SMEM),
        "vmem": lambda x: pltpu.with_memory_space_constraint(x, pltpu.VMEM),
        "hbm": lambda x: pltpu.with_memory_space_constraint(x, pltpu.HBM),
    }
    return pl.pallas_call(
        kernel,
        out_shape=[x for _, x in outs],
        in_specs=[spec[where] for where, _ in args],
        out_specs=[spec[where] for where, _ in outs],
        scratch_shapes=scratch,
        input_output_aliases=alias,
        compiler_params=pltpu.CompilerParams(vmem_limit_bytes=mib * MB),
        cost_estimate=pl.CostEstimate(flops=2 * 10**7, bytes_accessed=10**6, transcendentals=0),
    )(*(put[where](x) for where, x in args))


def ints(n):
    return ("smem", pltpu.SMEM((n,), jnp.int32))


def near(shape, dtype):
    return ("vmem", pltpu.VMEM(shape, dtype))


def code(x, scratch, row):
    top = jnp.maximum(jnp.max(jnp.abs(x), axis=0, keepdims=True), 1e-37)
    exponent = jnp.floor(jnp.log2(top)) + 1.0
    scratch[pl.ds(row, 1), :] = exponent
    return jnp.round(x * (jnp.exp2(-exponent) * LEVELS)).astype(jnp.int32).astype(jnp.int16)


def widen(x):
    return x.astype(jnp.int32).astype(jnp.float32)


def place_of(axis):
    return lax.axis_index(axis).astype(jnp.int32)


def started(sem, *pairs):
    copies = [pltpu.make_async_copy(src, dst, sem.at[n]) for n, (src, dst) in enumerate(pairs)]
    for c in copies:
        c.start()
    return copies


def plan_kernel(
    mine_hbm, their_vmem, pc_hbm, cc_hbm, tiles_hbm, p_hbm,
    entries, count, small, sidx, tiles, p, pt, acc,
    source, mine, their, pc, cc, sem,
):
    lanes = [pl.ds(n * T, T) for n in range(8)]
    copies = started(
        sem,
        (mine_hbm, mine),
        (their_vmem, their),
        (p_hbm, p.at[0]),
        *((pc_hbm.at[:, lanes[n]], pc.at[n]) for n in range(8)),
        *((cc_hbm.at[:, lanes[n]], cc.at[n]) for n in range(4)),
        (tiles_hbm, tiles.at[pl.ds(0, NA)]),
    )
    b, g = place_of("row"), place_of("grp")
    odd = lax.rem(b, 2)
    quarters = (g * KG, lax.rem(g + 2, G) * KG)
    for n in range(LISTS):
        count[n] = 0
        for u in range(FRONT):
            row = (n * CAP + u) * WORDS
            entries[row] = 0
            for k in range(KP):
                entries[row + 1 + k] = SPARE
    source[2] = 0
    source[1] = jnp.where(odd == 0, 3, 1)
    source[3] = jnp.where(odd == 0, 1, 3)
    source[0] = jnp.where(odd == 0, 4, 2)
    source[4] = jnp.where(odd == 0, 2, 4)
    for n in range(PLIST):
        small[n] = 0
    lowest = (b - 3) * C
    for c in copies[:-1]:
        c.wait()

    def rows(i, _):
        for w in range(NW):
            acc[i * NW + w] = jnp.zeros((T, T), jnp.float32)
        for which, cols in enumerate((mine, their)):
            for s in range(S):
                j = cols[s, 0, i]
                block = source[(j >> 3) - b + 2]
                if which == 0:
                    n = jnp.where(block == 0, 0, block - 1) + jnp.where(block > 2, 1, 0)
                else:
                    n = jnp.maximum(block, 2)
                at = count[n]
                count[n] = at + 1
                row = (n * CAP + FRONT + at) * WORDS
                entries[row] = (which * NA + i * S + s) | ((block * F + (j & (F - 1))) << 8)
                for k in range(KP):
                    entries[row + 1 + k] = pc[j >> 7, k, j & (T - 1)] + (i * NW - lowest)
        for q in range(KP):
            pr = i * KP + q
            pt[pr] = p[0, i, q].T
            f = b * F + i
            c = pc[f >> 7, q, f & (T - 1)]
            local = c - (b - 1) * C
            block = local >> 2
            kind = jnp.where(block == 1, 2, jnp.where((block == 0) == (odd == 0), 0, 1))
            crow = kind * C + (local & (C - 1))
            at = small[PAIRS + crow]
            small[PAIRS + crow] = at + 1
            small[PLIST + crow * (F * KP) + at] = pr
            for k in range(KD):
                w = cc[c >> 7, quarters[k // KG] + k % KG, c & (T - 1)] - lowest
                sidx[pr * KD + k] = jnp.where((w >= 0) & (w < NW), i * NW + w, ZERO)
        return 0

    lax.fori_loop(0, F, rows, 0)
    for n in range(LISTS):
        many = count[n]
        for u in range(2 * U - 1):
            row = (n * CAP + FRONT + many + u) * WORDS
            entries[row] = 0
            for k in range(KP):
                entries[row + 1 + k] = SPARE
        count[n] = (many + (2 * U - 1)) >> 3
    copies[-1].wait()


def planned(mine, their, p_cols, c_cols, a_tiles, p_tiles):
    mine, their = jnp.transpose(mine, (2, 1, 0)), jnp.transpose(their, (2, 1, 0))
    smem = lambda *shape: pltpu.SMEM(shape, jnp.int32)
    return call(
        plan_kernel,
        [("hbm", mine), ("vmem", their)] + [("hbm", x) for x in (p_cols.T, c_cols.T, a_tiles, p_tiles)],
        [
            ints(LISTS * CAP * WORDS),
            ints(8),
            ints(SMALL),
            ints(F * KP * KD),
            near((2 * NA, T, T), jnp.bfloat16),
            near((5, F, KP, T, T), jnp.bfloat16),
            near((F * KP, T, T), jnp.bfloat16),
            near((NS, T, T), jnp.float32),
        ],
        [
            smem(8),
            smem(*mine.shape),
            smem(*mine.shape),
            smem(8, KP, T),
            smem(4, KC, T),
            pltpu.SemaphoreType.DMA((16,)),
        ],
    )


def entry_loop(n, count, entries, a, p, acc, sets):
    zero = jnp.zeros((T, T), jnp.bfloat16)

    def issue(low, high, at, u):
        word = entries[at + u * WORDS]
        tile = a[word & 255]
        j = word >> 8
        block, r = j >> 3, j & (F - 1)
        rhs = jnp.concatenate(
            [jnp.concatenate([p[block, r, 2 * k], p[block, r, 2 * k + 1]], axis=1) for k in range(2)], axis=0
        )
        pltpu.matmul_push_rhs(rhs, staging_register=(u // 2) % 2, mxu_index=u % 2)
        pltpu.matmul_acc_lhs(low[u], jnp.concatenate([tile, zero], axis=1), load_staged_rhs=(u // 2) % 2)
        pltpu.matmul_acc_lhs(high[u], jnp.concatenate([zero, tile], axis=1))

    def drain(low, high, at, u):
        for k, ref in enumerate((low[u], high[u])):
            x = pltpu.matmul_pop(ref)
            for e in range(2):
                slot = entries[at + u * WORDS + 1 + 2 * k + e]
                acc[slot] += x[:, e * T : (e + 1) * T]

    def double(t, _):
        at = (n * CAP + FRONT + 2 * U * t) * WORDS
        for u in range(U):
            issue(*sets[0], at, u)
            drain(*sets[1], at - U * WORDS, u)
        for u in range(U):
            issue(*sets[1], at + U * WORDS, u)
            drain(*sets[0], at, u)
        return 0

    many = count[n]
    lax.fori_loop(0, many, double, 0)
    for u in range(U):
        drain(*sets[1], (n * CAP + 2 * U * many) * WORDS, u)


def with_sets(work):
    def body(*refs):
        refs = list(refs)
        sets = []
        for _ in range(2):
            sets.append(([refs.pop(0) for _ in range(U)], [refs.pop(0) for _ in range(U)]))
        for low, high in sets:
            for ref in (*low, *high):
                pltpu.matmul_pop(ref)
        work(sets)

    pl.run_scoped(body, *[pltpu.ACC(u % 2)((T, 2 * T), jnp.float32) for _ in range(4) for u in range(U)])


def part_kernel(lists, blocks, with_tiles, split, count, entries, *refs):
    refs = list(refs)
    tiles = refs.pop(0) if with_tiles else None
    new = [refs.pop(0) for _ in blocks]
    if split:
        a, p, acc, sp = refs[-4:]
    else:
        a, p, acc = refs[-3:]
    for block, ref in zip(blocks, new):
        p[block] = ref[...]
    if with_tiles:
        a[NA : 2 * NA] = tiles[...]

    def work(sets):
        for n in lists:
            entry_loop(n, count, entries, a, p, acc, sets)

    with_sets(work)
    if split:
        sp[ZERO] = jnp.zeros((2 * T, T), jnp.bfloat16)

        def halves(t, _):
            for u in range(4):
                n = t * 4 + u
                x = acc[n]
                hi = x.astype(jnp.bfloat16)
                sp[n, 0:T, :] = hi
                sp[n, T : 2 * T, :] = (x - hi.astype(jnp.float32)).astype(jnp.bfloat16)
            return 0

        lax.fori_loop(0, F * NW // 4, halves, 0)


def part(lists, tabs, state, blocks, tiles=None, split=False):
    args = [("smem", x) for x in tabs]
    if tiles is not None:
        args.append(("vmem", tiles))
    args += [("vmem", x) for x in blocks.values()]
    outs = [near((2 * NA, T, T), jnp.bfloat16), near((5, F, KP, T, T), jnp.bfloat16), near((NS, T, T), jnp.float32)]
    alias = {len(args) + n: n for n in range(len(state))}
    args += [("vmem", x) for x in state]
    if split:
        outs.append(near((NS, 2 * T, T), jnp.bfloat16))
    return call(functools.partial(part_kernel, lists, tuple(blocks), tiles is not None, split), args, outs, alias=alias)


def coarse_kernel(rows, small, sidx, sp, pt, *refs):
    outs, ex = refs[:-1], refs[-1]

    def body(*accs):
        for acc in accs:
            pltpu.matmul_pop(acc)
        for c, (kind, at, *half) in rows:
            out = outs[0].at[half[0]] if half else outs[0]
            e0 = half[0] * 2 * SCALES if half else 0

            def pair(r, _):
                pr = small[PLIST + c * (F * KP) + r]
                tile = pt[pr]
                lhs = jnp.concatenate([tile, tile], axis=1)
                for n in range(KD // 2):
                    rhs = jnp.concatenate([sp[sidx[pr * KD + 2 * n]], sp[sidx[pr * KD + 2 * n + 1]]], axis=1)
                    pltpu.matmul_push_rhs(rhs, staging_register=(n // 2) % 2, mxu_index=n % 2)
                    pltpu.matmul_acc_lhs(accs[n], lhs, load_staged_rhs=(n // 2) % 2)
                return 0

            lax.fori_loop(0, small[PAIRS + c], pair, 0)
            for n in range(KD // 2):
                x = pltpu.matmul_pop(accs[n])
                for e in range(2):
                    k = 2 * n + e
                    y = x[:, e * T : (e + 1) * T]
                    if kind == "plain":
                        out[at, k] = y
                    else:
                        d, t = k // KG, at * KG + k % KG
                        out[d, t * T : (t + 1) * T, :] = code(y, ex, e0 + d * SCALES + t)
            if kind == "code" and at == HC - 1:
                for d in range(2):
                    r0 = e0 + d * SCALES
                    out[d, ROWS:PACK, :] = ex[r0 : r0 + SCALES, :].astype(jnp.int32).astype(jnp.int16)

    pl.run_scoped(body, *[pltpu.ACC(n % 2)((T, 2 * T), jnp.float32) for n in range(KD // 2)])


def coarse(rows, out, tabs, sp, pt):
    return call(
        functools.partial(coarse_kernel, rows),
        [("smem", tabs[0]), ("smem", tabs[1]), ("vmem", sp), ("vmem", pt)],
        [out],
        [pltpu.VMEM((4 * SCALES, T), jnp.float32)],
    )[0]


def outer_chunk(h, *args):
    rows = [(HC * h + c, ("code", c)) for c in range(HC)]
    return coarse(rows, near((2, PACK, T), jnp.int16), *args)


def inner_chunks(*args):
    rows = [(C + HC * h + c, ("code", c, h)) for h in range(2) for c in range(HC)]
    return coarse(rows, near((2, 2, PACK, T), jnp.int16), *args)


def own_rows(h, *args):
    rows = [(2 * C + HC * h + c, ("plain", c)) for c in range(HC)]
    return coarse(rows, near((HC, KD, T, T), jnp.float32), *args)


def tiles():
    return [(c * KG + k, c, k, slice((c * KG + k) * T, (c * KG + k + 1) * T)) for c in range(HC) for k in range(KG)]


def sum_kernel(h, own, inner, outer, mine, send, ex_i, ex_o, ex):
    for d in (1, 0):
        ex_i[...] = jnp.exp2(widen(inner[h, d, ROWS:PACK, :])) * (1.0 / LEVELS)
        ex_o[...] = jnp.exp2(widen(outer[d, ROWS:PACK, :])) * (1.0 / LEVELS)
        for t, c, k, rows in tiles():
            x = own[c, d * KG + k] + widen(inner[h, d, rows, :]) * ex_i[t : t + 1, :]
            x = x + widen(outer[d, rows, :]) * ex_o[t : t + 1, :]
            if d:
                send[rows, :] = code(x, ex, t)
            else:
                mine[c, k] = x
        if d:
            send[ROWS:PACK, :] = ex[...].astype(jnp.int32).astype(jnp.int16)


def summed(h, own, inner, outer):
    return call(
        functools.partial(sum_kernel, h),
        [("vmem", x) for x in (own, inner, outer)],
        [near((HC, KG, T, T), jnp.float32), near((PACK, T), jnp.int16)],
        [pltpu.VMEM((SCALES, T), jnp.float32)] * 3,
    )


def final_kernel(*refs):
    out, ex = refs[-2:]
    for h in range(2):
        mine, got = refs[2 * h : 2 * h + 2]
        ex[...] = jnp.exp2(widen(got[ROWS:PACK, :])) * (1.0 / LEVELS)
        for t, c, k, rows in tiles():
            out[h * HC + c, k] = mine[c, k] + widen(got[rows, :]) * ex[t : t + 1, :]


def finished(parts):
    return call(
        final_kernel,
        [("vmem", x) for x in parts],
        [("vmem", jax.ShapeDtypeStruct((C, KG, T, T), jnp.float32))],
        [pltpu.VMEM((SCALES, T), jnp.float32)],
    )[0]


def along(x, to):
    n = lax.axis_size("row")
    return lax.ppermute(x, "row", [(i, to(i) % n) for i in range(n)])


def across(x, to):
    rows, n = lax.axis_size("row"), lax.axis_size("grp")
    return lax.ppermute(
        x, ("grp", "row"), [(g * rows + r, to(g, r % 2) * rows + r) for r in range(rows) for g in range(n)]
    )


def partner(g, core):
    return g ^ (3 if core else 1)


def opposite(g, core):
    return g ^ 2


def other(i):
    return i ^ 1


def away(i):
    return i - 1 if i % 2 == 0 else i + 1


def body(a_tiles, a_cols, p_tiles, p_cols, c_cols):
    tiles = a_tiles.reshape(NA, T, T)
    their_cols = across(a_cols, partner)
    turn = along(p_tiles, lambda i: i - 2 if i % 2 == 0 else i + 2)
    their_tiles = across(tiles, partner)
    beside = along(p_tiles, other)
    keep = along(p_tiles, lambda i: i + 2 if i % 2 == 0 else i - 2)
    entries, count, small, sidx, a, p, pt, acc = planned(a_cols, their_cols, p_cols, c_cols, tiles, p_tiles)
    lists, tabs, state = (count, entries), (small, sidx), (a, p, acc)
    state = part((0,), lists, state, {1: beside})
    far = along(turn, other)
    state = part((1,), lists, state, {2: turn})
    state = part((2, 3), lists, state, {3: far}, their_tiles)
    sp = part((4,), lists, state, {4: keep}, split=True)[3]
    out0 = outer_chunk(0, tabs, sp, pt)
    got0 = along(out0, away)
    ins = inner_chunks(tabs, sp, pt)
    out1 = outer_chunk(1, tabs, sp, pt)
    inner = along(ins, other)
    got1 = along(out1, away)
    parts = []
    for h, outer in enumerate((got0, got1)):
        own = own_rows(h, tabs, sp, pt)
        mine, send = summed(h, own, inner, outer)
        parts += [mine, across(send, opposite)]
    return finished(parts)


def solution(mesh):
    return jax.shard_map(
        body,
        mesh=mesh,
        in_specs=(
            P("row", "grp", None, None, None),
            P("row", "grp", None),
            P("row", None, None, None),
            P(),
            P(),
        ),
        out_specs=P("row", "grp", None, None),
        check_vma=False,
    )
```

```python
import functools

import jax
import jax.numpy as jnp
from jax import lax
from jax.experimental import pallas as pl
from jax.experimental.pallas import tpu as pltpu
from jax.sharding import PartitionSpec as P


T = 128
F = 8
C = 4
S = 7
KP = 4
KC = 16
G = 4
KG = KC // G
KD = 2 * KG
NA = F * S
SCALES = C * KG
ROWS = SCALES * T
PACK = ROWS + SCALES
LEVELS = 32760.0
MB = 1 << 20

NW = 7 * C
SPARE = F * NW
ZERO = SPARE + 1
NS = ZERO + 1

LISTS = 4
U = 4
FRONT = U
CAP = FRONT + 2 * NA + 2 * U
WORDS = 1 + KP
PAIRS, PLIST = 0, 16
SMALL = PLIST + 3 * C * F * KP

SMEM = pl.BlockSpec(memory_space=pltpu.SMEM)
VMEM = pl.BlockSpec(memory_space=pltpu.VMEM)
HBM = pl.BlockSpec(memory_space=pltpu.HBM)


def call(kernel, args, outs, scratch=(), alias={}, mib=4):
    spec = {"smem": SMEM, "vmem": VMEM, "hbm": HBM}
    put = {
        "smem": lambda x: pltpu.with_memory_space_constraint(x, pltpu.SMEM),
        "vmem": lambda x: pltpu.with_memory_space_constraint(x, pltpu.VMEM),
        "hbm": lambda x: pltpu.with_memory_space_constraint(x, pltpu.HBM),
    }
    return pl.pallas_call(
        kernel,
        out_shape=[x for _, x in outs],
        in_specs=[spec[where] for where, _ in args],
        out_specs=[spec[where] for where, _ in outs],
        scratch_shapes=scratch,
        input_output_aliases=alias,
        compiler_params=pltpu.CompilerParams(vmem_limit_bytes=mib * MB),
        cost_estimate=pl.CostEstimate(flops=2 * 10**7, bytes_accessed=10**6, transcendentals=0),
    )(*(put[where](x) for where, x in args))


def ints(n):
    return ("smem", pltpu.SMEM((n,), jnp.int32))


def near(shape, dtype):
    return ("vmem", pltpu.VMEM(shape, dtype))


def code(x, scratch, row):
    top = jnp.maximum(jnp.max(jnp.abs(x), axis=0, keepdims=True), 1e-37)
    exponent = jnp.floor(jnp.log2(top)) + 1.0
    scratch[pl.ds(row, 1), :] = exponent
    return jnp.round(x * (jnp.exp2(-exponent) * LEVELS)).astype(jnp.int32).astype(jnp.int16)


def widen(x):
    return x.astype(jnp.int32).astype(jnp.float32)


def place_of(axis):
    return lax.axis_index(axis).astype(jnp.int32)


def started(sem, *pairs):
    copies = [pltpu.make_async_copy(src, dst, sem.at[n]) for n, (src, dst) in enumerate(pairs)]
    for c in copies:
        c.start()
    return copies


def plan_kernel(
    mine_hbm, their_vmem, pc_hbm, cc_hbm, tiles_hbm, p_hbm,
    entries, count, small, sidx, tiles, p, pt, acc, sp,
    source, mine, their, pc, cc, sem,
):
    b, g = place_of("row"), place_of("grp")
    odd = lax.rem(b, 2)
    quarters = (jnp.where(odd == 0, 3 - g, g + 1 - 2 * (g & 1)) * KG, g * KG)
    np, nc = pc_hbm.shape[1], cc_hbm.shape[1]
    copies = started(
        sem,
        (mine_hbm, mine),
        (their_vmem, their),
        (p_hbm, p.at[0]),
        *((pc_hbm.at[k], pc.at[pl.ds(k * np, np)]) for k in range(KP)),
        *((cc_hbm.at[quarters[k // KG] + k % KG], cc.at[pl.ds(k * nc, nc)]) for k in range(KD)),
        (tiles_hbm, tiles.at[pl.ds(0, NA)]),
    )
    for n in range(LISTS):
        count[n] = 0
        for u in range(FRONT):
            row = (n * CAP + u) * WORDS
            entries[row] = 0
            for k in range(KP):
                entries[row + 1 + k] = SPARE
    source[2] = 0
    source[1] = jnp.where(odd == 0, 3, 1)
    source[3] = jnp.where(odd == 0, 1, 3)
    source[0] = jnp.where(odd == 0, 4, 2)
    source[4] = jnp.where(odd == 0, 2, 4)
    for n in range(PLIST):
        small[n] = 0
    lowest = (b - 3) * C

    def clear(n, _):
        for w in range(4):
            acc[n * 4 + w] = jnp.zeros((T, T), jnp.float32)
        return 0

    lax.fori_loop(0, F * NW // 4, clear, 0)
    sp[ZERO] = jnp.zeros((2 * T, T), jnp.bfloat16)
    for c in copies[:-1]:
        c.wait()

    for which, cols in enumerate((mine, their)):

        def enter(i, _):
            for s in range(S):
                j = cols[s, 0, i]
                block = source[(j >> 3) - b + 2]
                n = jnp.where(block < 2, which, 2 + (block >> 2))
                at = count[n]
                count[n] = at + 1
                row = (n * CAP + FRONT + at) * WORDS
                entries[row] = (which * NA + i * S + s) | ((block * F + (j & (F - 1))) << 8)
                for k in range(KP):
                    entries[row + 1 + k] = pc[k * np + j] + (i * NW - lowest)
            return 0

        lax.fori_loop(0, F, enter, 0)

    def pairs(i, _):
        for q in range(KP):
            pr = i * KP + q
            pt[pr] = p[0, i, q].T
            c = pc[q * np + b * F + i]
            local = c - (b - 1) * C
            block = local >> 2
            kind = jnp.where(block == 1, 2, jnp.where((block == 0) == (odd == 0), 0, 1))
            crow = kind * C + (local & (C - 1))
            at = small[PAIRS + crow]
            small[PAIRS + crow] = at + 1
            small[PLIST + crow * (F * KP) + at] = pr
            for k in range(KD):
                w = cc[k * nc + c] - lowest
                sidx[pr * KD + k] = jnp.where((w >= 0) & (w < NW), i * NW + w, ZERO)
        return 0

    lax.fori_loop(0, F, pairs, 0)
    for n in range(LISTS):
        many = count[n]
        for u in range(2 * U - 1):
            row = (n * CAP + FRONT + many + u) * WORDS
            entries[row] = 0
            for k in range(KP):
                entries[row + 1 + k] = SPARE
        count[n] = (many + (2 * U - 1)) >> 3
    copies[-1].wait()


def planned(mine, their, p_cols, c_cols, a_tiles, p_tiles):
    mine, their = jnp.transpose(mine, (2, 1, 0)), jnp.transpose(their, (2, 1, 0))
    smem = lambda *shape: pltpu.SMEM(shape, jnp.int32)
    return call(
        plan_kernel,
        [("hbm", mine), ("vmem", their)] + [("hbm", x) for x in (p_cols.T, c_cols.T, a_tiles, p_tiles)],
        [
            ints(LISTS * CAP * WORDS),
            ints(8),
            ints(SMALL),
            ints(F * KP * KD),
            near((2 * NA, T, T), jnp.bfloat16),
            near((5, F, KP, T, T), jnp.bfloat16),
            near((F * KP, T, T), jnp.bfloat16),
            near((NS, T, T), jnp.float32),
            near((NS, 2 * T, T), jnp.bfloat16),
        ],
        [
            smem(8),
            smem(*mine.shape),
            smem(*mine.shape),
            smem(p_cols.size),
            smem(c_cols.size // 2),
            pltpu.SemaphoreType.DMA((16,)),
        ],
    )


def entry_loop(n, count, entries, a, p, acc, sets):
    zero = jnp.zeros((T, T), jnp.bfloat16)

    def issue(low, high, at, u):
        word = entries[at + u * WORDS]
        tile = a[word & 255]
        j = word >> 8
        block, r = j >> 3, j & (F - 1)
        rhs = jnp.concatenate(
            [jnp.concatenate([p[block, r, 2 * k], p[block, r, 2 * k + 1]], axis=1) for k in range(2)], axis=0
        )
        pltpu.matmul_push_rhs(rhs, staging_register=(u // 2) % 2, mxu_index=u % 2)
        pltpu.matmul_acc_lhs(low[u], jnp.concatenate([tile, zero], axis=1), load_staged_rhs=(u // 2) % 2)
        pltpu.matmul_acc_lhs(high[u], jnp.concatenate([zero, tile], axis=1))

    def drain(low, high, at, u):
        for k, ref in enumerate((low[u], high[u])):
            x = pltpu.matmul_pop(ref)
            for e in range(2):
                slot = entries[at + u * WORDS + 1 + 2 * k + e]
                acc[slot] += x[:, e * T : (e + 1) * T]

    def double(t, _):
        at = (n * CAP + FRONT + 2 * U * t) * WORDS
        for u in range(U):
            issue(*sets[0], at, u)
            drain(*sets[1], at - U * WORDS, u)
        for u in range(U):
            issue(*sets[1], at + U * WORDS, u)
            drain(*sets[0], at, u)
        return 0

    many = count[n]
    lax.fori_loop(0, many, double, 0)
    for u in range(U):
        drain(*sets[1], (n * CAP + 2 * U * many) * WORDS, u)


def with_sets(work):
    def body(*refs):
        refs = list(refs)
        sets = []
        for _ in range(2):
            sets.append(([refs.pop(0) for _ in range(U)], [refs.pop(0) for _ in range(U)]))
        for low, high in sets:
            for ref in (*low, *high):
                pltpu.matmul_pop(ref)
        work(sets)

    pl.run_scoped(body, *[pltpu.ACC(u % 2)((T, 2 * T), jnp.float32) for _ in range(4) for u in range(U)])


def part_kernel(lists, blocks, with_tiles, halve, count, entries, *refs):
    refs = list(refs)
    their = refs.pop(0) if with_tiles else None
    new = [refs.pop(0) for _ in blocks]
    a, p, acc, sp = refs[-4:]
    for block, ref in zip(blocks, new):
        p[block] = ref[...]
    if with_tiles:
        a[NA : 2 * NA] = their[...]

    def work(sets):
        for n in lists:
            entry_loop(n, count, entries, a, p, acc, sets)

    with_sets(work)
    if halve:
        odd = lax.rem(place_of("row"), 2)
        if halve == "most":
            start, width = (1 - odd) * 3 * C, 4 * C
        else:
            start, width = odd * 4 * C, 3 * C

        def halves(t, _):
            first = (t >> 2) * NW + start + (t & 3) * (width // 4)
            for u in range(width // 4):
                x = acc[first + u]
                hi = x.astype(jnp.bfloat16)
                sp[first + u, 0:T, :] = hi
                sp[first + u, T : 2 * T, :] = (x - hi.astype(jnp.float32)).astype(jnp.bfloat16)
            return 0

        lax.fori_loop(0, 4 * F, halves, 0)


def part(lists, tabs, state, blocks, tiles=None, halve=None):
    args = [("smem", x) for x in tabs]
    if tiles is not None:
        args.append(("vmem", tiles))
    args += [("vmem", x) for x in blocks.values()]
    outs = [near(x.shape, x.dtype) for x in state]
    alias = {len(args) + n: n for n in range(len(state))}
    args += [("vmem", x) for x in state]
    return call(functools.partial(part_kernel, lists, tuple(blocks), tiles is not None, halve), args, outs, alias=alias)


def coarse_kernel(first, quarters, coded, small, sidx, sp, pt, out, *refs):
    def body(*accs):
        for acc in accs:
            pltpu.matmul_pop(acc)
        for c in range(C):

            def pair(r, _):
                pr = small[PLIST + (first + c) * (F * KP) + r]
                tile = pt[pr]
                lhs = jnp.concatenate([tile, tile], axis=1)
                for n, acc in enumerate(accs):
                    k = pr * KD + quarters[0] * KG + 2 * n
                    rhs = jnp.concatenate([sp[sidx[k]], sp[sidx[k + 1]]], axis=1)
                    pltpu.matmul_push_rhs(rhs, staging_register=(n // 2) % 2, mxu_index=n % 2)
                    pltpu.matmul_acc_lhs(acc, lhs, load_staged_rhs=(n // 2) % 2)
                return 0

            lax.fori_loop(0, small[PAIRS + first + c], pair, 0)
            for n, acc in enumerate(accs):
                x = pltpu.matmul_pop(acc)
                for e in range(2):
                    q, k = divmod(2 * n + e, KG)
                    y = x[:, e * T : (e + 1) * T]
                    if coded:
                        t = c * KG + k
                        out[q, t * T : (t + 1) * T, :] = code(y, refs[0].at[q], t)
                    else:
                        out[c, k] = y
        if coded:
            for q in range(len(quarters)):
                out[q, ROWS:PACK, :] = refs[0][q].astype(jnp.int32).astype(jnp.int16)

    pl.run_scoped(body, *[pltpu.ACC(n % 2)((T, 2 * T), jnp.float32) for n in range(len(quarters) * KG // 2)])


OUTER, INNER, OWN = 0, C, 2 * C


def coarse(first, quarters, coded, tabs, sp, pt):
    n = len(quarters)
    out = near((n, PACK, T), jnp.int16) if coded else near((C, KG, T, T), jnp.float32)
    return call(
        functools.partial(coarse_kernel, first, quarters, coded),
        [("smem", tabs[0]), ("smem", tabs[1]), ("vmem", sp), ("vmem", pt)],
        [out],
        [pltpu.VMEM((n, SCALES, T), jnp.float32)] if coded else [],
    )[0]


def tiles():
    return [(c * KG + k, c, k, slice((c * KG + k) * T, (c * KG + k + 1) * T)) for c in range(C) for k in range(KG)]


def scale(ref, rows):
    ref[...] = jnp.exp2(widen(rows)) * (1.0 / LEVELS)


def cross_kernel(inner, outer, out, ex_i, ex_o, ex):
    scale(ex_i, inner[0, ROWS:PACK, :])
    scale(ex_o, outer[0, ROWS:PACK, :])
    for t, c, k, rows in tiles():
        x = widen(inner[0, rows, :]) * ex_i[t : t + 1, :] + widen(outer[0, rows, :]) * ex_o[t : t + 1, :]
        out[0, rows, :] = code(x, ex, t)
    out[0, ROWS:PACK, :] = ex[...].astype(jnp.int32).astype(jnp.int16)


def crossed(inner, outer):
    return call(
        cross_kernel,
        [("vmem", inner), ("vmem", outer)],
        [near((1, PACK, T), jnp.int16)],
        [pltpu.VMEM((SCALES, T), jnp.float32)] * 3,
    )[0]


def add_kernel(own, *refs):
    *coded, out, ex = refs
    coded = [x.at[x.shape[0] - 1] for x in coded]
    for n, x in enumerate(coded):
        scale(ex.at[n], x[ROWS:PACK, :])
    for t, c, k, rows in tiles():
        y = own[c, k]
        for n, x in enumerate(coded):
            y = y + widen(x[rows, :]) * ex[n, t : t + 1, :]
        out[c, k] = y


def added(own, coded, out):
    return call(
        add_kernel,
        [("vmem", x) for x in (own, *coded)],
        [("vmem", out)],
        [pltpu.VMEM((len(coded), SCALES, T), jnp.float32)],
    )[0]


def along(x, to):
    n = lax.axis_size("row")
    return lax.ppermute(x, "row", [(i, to(i) % n) for i in range(n)])


def across(x, to):
    rows, n = lax.axis_size("row"), lax.axis_size("grp")
    return lax.ppermute(
        x, ("grp", "row"), [(g * rows + r, to(g, r % 2) * rows + r) for r in range(rows) for g in range(n)]
    )


def partner(g, core):
    return g ^ (3 if core else 1)


def second(g, core):
    return partner(g, 1 - core)


def other(i):
    return i ^ 1


def away(i):
    return i - 1 if i % 2 == 0 else i + 1


def body(a_tiles, a_cols, p_tiles, p_cols, c_cols):
    tiles = a_tiles.reshape(NA, T, T)
    their_cols = across(a_cols, partner)
    their_tiles = across(tiles, partner)
    turn = along(p_tiles, lambda i: i - 2 if i % 2 == 0 else i + 2)
    beside = along(p_tiles, other)
    keep = along(p_tiles, lambda i: i + 2 if i % 2 == 0 else i - 2)
    entries, count, small, sidx, a, p, pt, acc, sp = planned(
        a_cols, their_cols, p_cols, c_cols, tiles, p_tiles
    )
    lists, state = (count, entries), (a, p, acc, sp)
    state = part((0,), lists, state, {1: beside})
    far = along(turn, other)
    state = part((1,), lists, state, {}, their_tiles)
    state = part((2,), lists, state, {2: turn, 3: far}, halve="most")
    sp = part((3,), lists, state, {4: keep}, halve="rest")[3]
    rows = ((small, sidx), sp, pt)
    x = coarse(OUTER, (0,), True, *rows)
    outer = along(x, away)
    x = coarse(INNER, (0, 1), True, *rows)
    inner = along(x, other)
    x = coarse(OWN, (0,), True, *rows)
    from_second = across(x, second)
    x = crossed(inner, outer)
    from_partner = across(x, partner)
    x = coarse(OUTER, (1,), True, *rows)
    outer = along(x, away)
    own = coarse(OWN, (1,), False, *rows)
    shape = (C, KG, T, T)
    mine = added(own, (inner, outer), pltpu.VMEM(shape, jnp.float32))
    return added(mine, (from_second, from_partner), jax.ShapeDtypeStruct(shape, jnp.float32))


def solution(mesh):
    return jax.shard_map(
        body,
        mesh=mesh,
        in_specs=(
            P("row", "grp", None, None, None),
            P("row", "grp", None),
            P("row", None, None, None),
            P(),
            P(),
        ),
        out_specs=P("row", "grp", None, None),
        check_vma=False,
    )
```

```python
import functools

import jax
import jax.numpy as jnp
from jax import lax
from jax.experimental import pallas as pl
from jax.experimental.pallas import tpu as pltpu
from jax.sharding import PartitionSpec as P


T = 128
F = 8
C = 4
S = 7
KP = 4
KC = 16
G = 4
KG = KC // G
KD = 2 * KG
NA = F * S
SCALES = C * KG
ROWS = SCALES * T
PACK = ROWS + SCALES
LEVELS = 32760.0
MB = 1 << 20

NW = 7 * C
SPARE = F * NW
ZERO = SPARE + 1
NS = ZERO + 1

LISTS = 4
U = 4
FRONT = U
CAP = FRONT + NA + 2 * U
WORDS = 1 + KP
PAIRS, PLIST = 0, 16
SMALL = PLIST + 3 * C * F * KP

SMEM = pl.BlockSpec(memory_space=pltpu.SMEM)
VMEM = pl.BlockSpec(memory_space=pltpu.VMEM)
HBM = pl.BlockSpec(memory_space=pltpu.HBM)


def call(kernel, args, outs, scratch=(), alias={}, mib=4):
    spec = {"smem": SMEM, "vmem": VMEM, "hbm": HBM}
    put = {
        "smem": lambda x: pltpu.with_memory_space_constraint(x, pltpu.SMEM),
        "vmem": lambda x: pltpu.with_memory_space_constraint(x, pltpu.VMEM),
        "hbm": lambda x: pltpu.with_memory_space_constraint(x, pltpu.HBM),
    }
    return pl.pallas_call(
        kernel,
        out_shape=[x for _, x in outs],
        in_specs=[spec[where] for where, _ in args],
        out_specs=[spec[where] for where, _ in outs],
        scratch_shapes=scratch,
        input_output_aliases=alias,
        compiler_params=pltpu.CompilerParams(vmem_limit_bytes=mib * MB),
        cost_estimate=pl.CostEstimate(flops=2 * 10**7, bytes_accessed=10**6, transcendentals=0),
    )(*(put[where](x) for where, x in args))


def ints(n):
    return ("smem", pltpu.SMEM((n,), jnp.int32))


def near(shape, dtype):
    return ("vmem", pltpu.VMEM(shape, dtype))


def code(x, scratch, row):
    top = jnp.maximum(jnp.max(jnp.abs(x), axis=0, keepdims=True), 1e-37)
    exponent = jnp.floor(jnp.log2(top)) + 1.0
    scratch[pl.ds(row, 1), :] = exponent
    return jnp.round(x * (jnp.exp2(-exponent) * LEVELS)).astype(jnp.int32).astype(jnp.int16)


def widen(x):
    return x.astype(jnp.int32).astype(jnp.float32)


def place_of(axis):
    return lax.axis_index(axis).astype(jnp.int32)


def started(sem, *pairs):
    copies = [pltpu.make_async_copy(src, dst, sem.at[n]) for n, (src, dst) in enumerate(pairs)]
    for c in copies:
        c.start()
    return copies


def plan_kernel(
    mine_hbm, their_vmem, pc_hbm, cc_hbm, tiles_hbm, p_hbm,
    entries, count, small, sidx, tiles, p, pt, acc, sp,
    source, mine, their, pc, cc, sem,
):
    b, g = place_of("row"), place_of("grp")
    odd = lax.rem(b, 2)
    quarters = (jnp.where(odd == 0, 3 - g, g + 1 - 2 * (g & 1)) * KG, g * KG)
    np, nc = pc_hbm.shape[1], cc_hbm.shape[1]
    copies = started(
        sem,
        (mine_hbm, mine),
        (their_vmem, their),
        (p_hbm, p.at[0]),
        *((pc_hbm.at[k], pc.at[pl.ds(k * np, np)]) for k in range(KP)),
        *((cc_hbm.at[quarters[k // KG] + k % KG], cc.at[pl.ds(k * nc, nc)]) for k in range(KD)),
        (tiles_hbm, tiles),
    )
    for n in range(LISTS):
        count[n] = 0
        for u in range(FRONT):
            row = (n * CAP + u) * WORDS
            entries[row] = 0
            for k in range(KP):
                entries[row + 1 + k] = SPARE
    source[2] = 0
    source[1] = jnp.where(odd == 0, 3, 1)
    source[3] = jnp.where(odd == 0, 1, 3)
    source[0] = jnp.where(odd == 0, 4, 2)
    source[4] = jnp.where(odd == 0, 2, 4)
    for n in range(PLIST):
        small[n] = 0
    lowest = (b - 3) * C

    def clear(n, _):
        for w in range(4):
            acc[n * 4 + w] = jnp.zeros((T, T), jnp.float32)
        return 0

    lax.fori_loop(0, F * NW // 4, clear, 0)
    sp[ZERO] = jnp.zeros((2 * T, T), jnp.bfloat16)
    for c in copies[:-1]:
        c.wait()

    for which, cols in enumerate((mine, their)):

        def enter(i, _):
            for s in range(S):
                j = cols[s, 0, i]
                block = source[(j >> 3) - b + 2]
                n = 3 if which else block >> 1
                at = count[n]
                count[n] = at + 1
                row = (n * CAP + FRONT + at) * WORDS
                entries[row] = (i * S + s) | ((block * F + (j & (F - 1))) << 8)
                for k in range(KP):
                    entries[row + 1 + k] = pc[k * np + j] + (i * NW - lowest)
            return 0

        lax.fori_loop(0, F, enter, 0)

    def pairs(i, _):
        for q in range(KP):
            pr = i * KP + q
            pt[pr] = p[0, i, q].T
            c = pc[q * np + b * F + i]
            local = c - (b - 1) * C
            block = local >> 2
            kind = jnp.where(block == 1, 2, jnp.where((block == 0) == (odd == 0), 0, 1))
            crow = kind * C + (local & (C - 1))
            at = small[PAIRS + crow]
            small[PAIRS + crow] = at + 1
            small[PLIST + crow * (F * KP) + at] = pr
            for k in range(KD):
                w = cc[k * nc + c] - lowest
                sidx[pr * KD + k] = jnp.where((w >= 0) & (w < NW), i * NW + w, ZERO)
        return 0

    lax.fori_loop(0, F, pairs, 0)
    for n in range(LISTS):
        many = count[n]
        for u in range(2 * U - 1):
            row = (n * CAP + FRONT + many + u) * WORDS
            entries[row] = 0
            for k in range(KP):
                entries[row + 1 + k] = SPARE
        count[n] = (many + (2 * U - 1)) >> 3
    copies[-1].wait()


def planned(mine, their, p_cols, c_cols, a_tiles, p_tiles):
    mine, their = jnp.transpose(mine, (2, 1, 0)), jnp.transpose(their, (2, 1, 0))
    smem = lambda *shape: pltpu.SMEM(shape, jnp.int32)
    return call(
        plan_kernel,
        [("hbm", mine), ("vmem", their)] + [("hbm", x) for x in (p_cols.T, c_cols.T, a_tiles, p_tiles)],
        [
            ints(LISTS * CAP * WORDS),
            ints(8),
            ints(SMALL),
            ints(F * KP * KD),
            near((NA, T, T), jnp.bfloat16),
            near((5, F, KP, T, T), jnp.bfloat16),
            near((F * KP, T, T), jnp.bfloat16),
            near((NS, T, T), jnp.float32),
            near((NS, 2 * T, T), jnp.bfloat16),
        ],
        [
            smem(8),
            smem(*mine.shape),
            smem(*mine.shape),
            smem(p_cols.size),
            smem(c_cols.size // 2),
            pltpu.SemaphoreType.DMA((16,)),
        ],
    )


def entry_loop(n, count, entries, a, p, acc, sets):
    zero = jnp.zeros((T, T), jnp.bfloat16)

    def issue(low, high, at, u):
        word = entries[at + u * WORDS]
        tile = a[word & 255]
        j = word >> 8
        block, r = j >> 3, j & (F - 1)
        rhs = jnp.concatenate(
            [jnp.concatenate([p[block, r, 2 * k], p[block, r, 2 * k + 1]], axis=1) for k in range(2)], axis=0
        )
        pltpu.matmul_push_rhs(rhs, staging_register=(u // 2) % 2, mxu_index=u % 2)
        pltpu.matmul_acc_lhs(low[u], jnp.concatenate([tile, zero], axis=1), load_staged_rhs=(u // 2) % 2)
        pltpu.matmul_acc_lhs(high[u], jnp.concatenate([zero, tile], axis=1))

    def drain(low, high, at, u):
        for k, ref in enumerate((low[u], high[u])):
            x = pltpu.matmul_pop(ref)
            for e in range(2):
                slot = entries[at + u * WORDS + 1 + 2 * k + e]
                acc[slot] += x[:, e * T : (e + 1) * T]

    def double(t, _):
        at = (n * CAP + FRONT + 2 * U * t) * WORDS
        for u in range(U):
            issue(*sets[0], at, u)
            drain(*sets[1], at - U * WORDS, u)
        for u in range(U):
            issue(*sets[1], at + U * WORDS, u)
            drain(*sets[0], at, u)
        return 0

    many = count[n]
    lax.fori_loop(0, many, double, 0)
    for u in range(U):
        drain(*sets[1], (n * CAP + 2 * U * many) * WORDS, u)


def with_sets(work):
    def body(*refs):
        refs = list(refs)
        sets = []
        for _ in range(2):
            sets.append(([refs.pop(0) for _ in range(U)], [refs.pop(0) for _ in range(U)]))
        for low, high in sets:
            for ref in (*low, *high):
                pltpu.matmul_pop(ref)
        work(sets)

    pl.run_scoped(body, *[pltpu.ACC(u % 2)((T, 2 * T), jnp.float32) for _ in range(4) for u in range(U)])


OUTER, INNER, OWN = 0, C, 2 * C


def form_rows(first, quarters, coded, accs, small, sidx, sp, pt, out, *ex):
    for c in range(C):

        def pair(r, _):
            pr = small[PLIST + (first + c) * (F * KP) + r]
            tile = pt[pr]
            lhs = jnp.concatenate([tile, tile], axis=1)
            for n, acc in enumerate(accs):
                k = pr * KD + quarters[0] * KG + 2 * n
                rhs = jnp.concatenate([sp[sidx[k]], sp[sidx[k + 1]]], axis=1)
                pltpu.matmul_push_rhs(rhs, staging_register=(n // 2) % 2, mxu_index=n % 2)
                pltpu.matmul_acc_lhs(acc, lhs, load_staged_rhs=(n // 2) % 2)
            return 0

        lax.fori_loop(0, small[PAIRS + first + c], pair, 0)
        for n, acc in enumerate(accs):
            x = pltpu.matmul_pop(acc)
            for e in range(2):
                q, k = divmod(2 * n + e, KG)
                y = x[:, e * T : (e + 1) * T]
                if coded:
                    t = c * KG + k
                    out[q, t * T : (t + 1) * T, :] = code(y, ex[0].at[q], t)
                else:
                    out[c, k] = y
    if coded:
        for q in range(len(quarters)):
            out[q, ROWS:PACK, :] = ex[0][q].astype(jnp.int32).astype(jnp.int16)


def part_kernel(n, blocks, count, entries, *refs):
    new = refs[: len(blocks)]
    a, p, acc, _ = refs[-4:]
    for block, ref in zip(blocks, new):
        p[block] = ref[...]
    with_sets(lambda sets: entry_loop(n, count, entries, a, p, acc, sets))


def part(n, tabs, state, blocks):
    args = [("smem", x) for x in tabs] + [("vmem", x) for x in (*blocks.values(), *state)]
    first = len(args) - len(state)
    return call(
        functools.partial(part_kernel, n, tuple(blocks)),
        args,
        [near(x.shape, x.dtype) for x in state],
        alias={first + n: n for n in range(len(state))},
    )


def last_kernel(count, entries, small, sidx, their, pt, *refs):
    _, p, acc, sp, out, ex = refs[-6:]

    def halves(t, _):
        for u in range(4):
            n = t * 4 + u
            x = acc[n]
            hi = x.astype(jnp.bfloat16)
            sp[n, 0:T, :] = hi
            sp[n, T : 2 * T, :] = (x - hi.astype(jnp.float32)).astype(jnp.bfloat16)
        return 0

    def work(sets):
        entry_loop(LISTS - 1, count, entries, their, p, acc, sets)
        lax.fori_loop(0, F * NW // 4, halves, 0)
        form_rows(OUTER, (0,), True, sets[0][0][:2], small, sidx, sp, pt, out, ex)

    with_sets(work)


def last(lists, tabs, state, their, pt):
    args = [("smem", x) for x in (*lists, *tabs)] + [("vmem", x) for x in (their, pt, *state)]
    first = len(args) - len(state)
    return call(
        last_kernel,
        args,
        [near(x.shape, x.dtype) for x in state] + [near((1, PACK, T), jnp.int16)],
        [pltpu.VMEM((1, SCALES, T), jnp.float32)],
        alias={first + n: n for n in range(len(state))},
    )[3:]


def coarse_kernel(first, quarters, coded, small, sidx, sp, pt, out, *ex):
    def body(*accs):
        for acc in accs:
            pltpu.matmul_pop(acc)
        form_rows(first, quarters, coded, accs, small, sidx, sp, pt, out, *ex)

    pl.run_scoped(body, *[pltpu.ACC(n % 2)((T, 2 * T), jnp.float32) for n in range(len(quarters) * KG // 2)])


def coarse(first, quarters, coded, tabs, sp, pt):
    n = len(quarters)
    out = near((n, PACK, T), jnp.int16) if coded else near((C, KG, T, T), jnp.float32)
    return call(
        functools.partial(coarse_kernel, first, quarters, coded),
        [("smem", tabs[0]), ("smem", tabs[1]), ("vmem", sp), ("vmem", pt)],
        [out],
        [pltpu.VMEM((n, SCALES, T), jnp.float32)] if coded else [],
    )[0]


def tiles():
    return [(c * KG + k, c, k, slice((c * KG + k) * T, (c * KG + k + 1) * T)) for c in range(C) for k in range(KG)]


def scale(ref, rows):
    ref[...] = jnp.exp2(widen(rows)) * (1.0 / LEVELS)


def cross_kernel(inner, outer, out, ex_i, ex_o, ex):
    scale(ex_i, inner[0, ROWS:PACK, :])
    scale(ex_o, outer[0, ROWS:PACK, :])
    for t, c, k, rows in tiles():
        x = widen(inner[0, rows, :]) * ex_i[t : t + 1, :] + widen(outer[0, rows, :]) * ex_o[t : t + 1, :]
        out[0, rows, :] = code(x, ex, t)
    out[0, ROWS:PACK, :] = ex[...].astype(jnp.int32).astype(jnp.int16)


def crossed(inner, outer):
    return call(
        cross_kernel,
        [("vmem", inner), ("vmem", outer)],
        [near((1, PACK, T), jnp.int16)],
        [pltpu.VMEM((SCALES, T), jnp.float32)] * 3,
    )[0]


def add_kernel(own, *refs):
    *coded, out, ex = refs
    coded = [x.at[x.shape[0] - 1] for x in coded]
    for n, x in enumerate(coded):
        scale(ex.at[n], x[ROWS:PACK, :])
    for t, c, k, rows in tiles():
        y = own[c, k]
        for n, x in enumerate(coded):
            y = y + widen(x[rows, :]) * ex[n, t : t + 1, :]
        out[c, k] = y


def added(own, coded):
    return call(
        add_kernel,
        [("vmem", x) for x in (own, *coded)],
        [near(own.shape, own.dtype)],
        [pltpu.VMEM((len(coded), SCALES, T), jnp.float32)],
    )[0]


def finish_kernel(own, *refs):
    *coded, out_hbm, out, ex, sem = refs
    coded = [x.at[x.shape[0] - 1] for x in coded]
    for n, x in enumerate(coded):
        scale(ex.at[n], x[ROWS:PACK, :])
    copies = [pltpu.make_async_copy(out.at[c], out_hbm.at[c], sem.at[c]) for c in range(C)]
    for t, c, k, rows in tiles():
        y = own[c, k]
        for n, x in enumerate(coded):
            y = y + widen(x[rows, :]) * ex[n, t : t + 1, :]
        out[c, k] = y
        if k == KG - 1:
            copies[c].start()
    for copy in copies:
        copy.wait()


def finished(own, coded):
    return call(
        finish_kernel,
        [("vmem", x) for x in (own, *coded)],
        [("hbm", jax.ShapeDtypeStruct(own.shape, own.dtype))],
        [
            pltpu.VMEM(own.shape, own.dtype),
            pltpu.VMEM((len(coded), SCALES, T), jnp.float32),
            pltpu.SemaphoreType.DMA((C,)),
        ],
    )[0]


def along(x, to):
    n = lax.axis_size("row")
    return lax.ppermute(x, "row", [(i, to(i) % n) for i in range(n)])


def across(x, to):
    rows, n = lax.axis_size("row"), lax.axis_size("grp")
    return lax.ppermute(
        x, ("grp", "row"), [(g * rows + r, to(g, r % 2) * rows + r) for r in range(rows) for g in range(n)]
    )


def partner(g, core):
    return g ^ (3 if core else 1)


def second(g, core):
    return partner(g, 1 - core)


def other(i):
    return i ^ 1


def away(i):
    return i - 1 if i % 2 == 0 else i + 1


def body(a_tiles, a_cols, p_tiles, p_cols, c_cols):
    tiles = a_tiles.reshape(NA, T, T)
    their_cols = across(a_cols, partner)
    their_tiles = across(tiles, partner)
    turn = along(p_tiles, lambda i: i - 2 if i % 2 == 0 else i + 2)
    beside = along(p_tiles, other)
    keep = along(p_tiles, lambda i: i + 2 if i % 2 == 0 else i - 2)
    entries, count, small, sidx, a, p, pt, acc, sp = planned(
        a_cols, their_cols, p_cols, c_cols, tiles, p_tiles
    )
    lists, state = (count, entries), (a, p, acc, sp)
    state = part(0, lists, state, {1: beside})
    far = along(turn, other)
    state = part(1, lists, state, {2: turn, 3: far})
    state = part(2, lists, state, {4: keep})
    sp, x = last(lists, (small, sidx), state, their_tiles, pt)
    rows = ((small, sidx), sp, pt)
    outer = along(x, away)
    x = coarse(INNER, (0, 1), True, *rows)
    inner = along(x, other)
    x = coarse(OWN, (0,), True, *rows)
    from_second = across(x, second)
    x = crossed(inner, outer)
    from_partner = across(x, partner)
    x = coarse(OUTER, (1,), True, *rows)
    outer = along(x, away)
    own = coarse(OWN, (1,), False, *rows)
    mine = added(own, (inner, outer))
    return finished(mine, (from_second, from_partner))


def solution(mesh):
    return jax.shard_map(
        body,
        mesh=mesh,
        in_specs=(
            P("row", "grp", None, None, None),
            P("row", "grp", None),
            P("row", None, None, None),
            P(),
            P(),
        ),
        out_specs=P("row", "grp", None, None),
        check_vma=False,
    )
```

```python
import functools

import jax
import jax.numpy as jnp
from jax import lax
from jax.experimental import pallas as pl
from jax.experimental.pallas import tpu as pltpu
from jax.sharding import PartitionSpec as P


T = 128
F = 8
C = 4
S = 7
KP = 4
KC = 16
G = 4
KG = KC // G
KD = 2 * KG
NA = F * S
SCALES = C * KG
ROWS = SCALES * T
PACK = ROWS + SCALES
LEVELS = 32760.0
MB = 1 << 20

NW = 7 * C
SPARE = F * NW
ZERO = SPARE + 1
NS = ZERO + 1

LISTS = 4
U = 4
FRONT = U
CAP = FRONT + NA + 2 * U
WORDS = 1 + KP
PAIRS, PLIST = 0, 16
SMALL = PLIST + 3 * C * F * KP

SMEM = pl.BlockSpec(memory_space=pltpu.SMEM)
VMEM = pl.BlockSpec(memory_space=pltpu.VMEM)
HBM = pl.BlockSpec(memory_space=pltpu.HBM)


def call(kernel, args, outs, scratch=(), alias={}, mib=4):
    spec = {"smem": SMEM, "vmem": VMEM, "hbm": HBM}
    put = {
        "smem": lambda x: pltpu.with_memory_space_constraint(x, pltpu.SMEM),
        "vmem": lambda x: pltpu.with_memory_space_constraint(x, pltpu.VMEM),
        "hbm": lambda x: pltpu.with_memory_space_constraint(x, pltpu.HBM),
    }
    return pl.pallas_call(
        kernel,
        out_shape=[x for _, x in outs],
        in_specs=[spec[where] for where, _ in args],
        out_specs=[spec[where] for where, _ in outs],
        scratch_shapes=scratch,
        input_output_aliases=alias,
        compiler_params=pltpu.CompilerParams(vmem_limit_bytes=mib * MB),
        cost_estimate=pl.CostEstimate(flops=2 * 10**7, bytes_accessed=10**6, transcendentals=0),
    )(*(put[where](x) for where, x in args))


def ints(n):
    return ("smem", pltpu.SMEM((n,), jnp.int32))


def near(shape, dtype):
    return ("vmem", pltpu.VMEM(shape, dtype))


def code(x, scratch, row):
    top = jnp.maximum(jnp.max(jnp.abs(x), axis=0, keepdims=True), 1e-37)
    exponent = jnp.floor(jnp.log2(top)) + 1.0
    scratch[pl.ds(row, 1), :] = exponent
    return jnp.round(x * (jnp.exp2(-exponent) * LEVELS)).astype(jnp.int32).astype(jnp.int16)


def widen(x):
    return x.astype(jnp.int32).astype(jnp.float32)


def place_of(axis):
    return lax.axis_index(axis).astype(jnp.int32)


def started(sem, *pairs):
    copies = [pltpu.make_async_copy(src, dst, sem.at[n]) for n, (src, dst) in enumerate(pairs)]
    for c in copies:
        c.start()
    return copies


def plan_kernel(
    mine_hbm, their_vmem, pc_hbm, cc_hbm, tiles_hbm, p_hbm,
    entries, count, small, sidx, tiles, p, pt, acc, sp,
    source, mine, their, pc, cc, sem,
):
    b, g = place_of("row"), place_of("grp")
    odd = lax.rem(b, 2)
    quarters = (jnp.where(odd == 0, 3 - g, g + 1 - 2 * (g & 1)) * KG, g * KG)
    np, nc = pc_hbm.shape[1], cc_hbm.shape[1]
    copies = started(
        sem,
        (mine_hbm, mine),
        (their_vmem, their),
        (p_hbm, p.at[0]),
        *((pc_hbm.at[k], pc.at[pl.ds(k * np, np)]) for k in range(KP)),
        *((cc_hbm.at[quarters[k // KG] + k % KG], cc.at[pl.ds(k * nc, nc)]) for k in range(KD)),
        (tiles_hbm, tiles),
    )
    for n in range(LISTS):
        count[n] = 0
        for u in range(FRONT):
            row = (n * CAP + u) * WORDS
            entries[row] = 0
            for k in range(KP):
                entries[row + 1 + k] = SPARE
    source[2] = 0
    source[1] = jnp.where(odd == 0, 3, 1)
    source[3] = jnp.where(odd == 0, 1, 3)
    source[0] = jnp.where(odd == 0, 4, 2)
    source[4] = jnp.where(odd == 0, 2, 4)
    for n in range(PLIST):
        small[n] = 0
    lowest = (b - 3) * C

    def clear(n, _):
        for w in range(4):
            acc[n * 4 + w] = jnp.zeros((T, T), jnp.float32)
        return 0

    lax.fori_loop(0, F * NW // 4, clear, 0)
    sp[ZERO] = jnp.zeros((2 * T, T), jnp.bfloat16)
    for c in copies[:-1]:
        c.wait()

    for which, cols in enumerate((mine, their)):

        def enter(i, _):
            for s in range(S):
                j = cols[s, 0, i]
                block = source[(j >> 3) - b + 2]
                n = 3 if which else block >> 1
                at = count[n]
                count[n] = at + 1
                row = (n * CAP + FRONT + at) * WORDS
                entries[row] = (i * S + s) | ((block * F + (j & (F - 1))) << 8)
                for k in range(KP):
                    entries[row + 1 + k] = pc[k * np + j] + (i * NW - lowest)
            return 0

        lax.fori_loop(0, F, enter, 0)

    def pairs(i, _):
        for q in range(KP):
            pr = i * KP + q
            pt[pr] = p[0, i, q].T
            c = pc[q * np + b * F + i]
            local = c - (b - 1) * C
            block = local >> 2
            kind = jnp.where(block == 1, 2, jnp.where((block == 0) == (odd == 0), 0, 1))
            crow = kind * C + (local & (C - 1))
            at = small[PAIRS + crow]
            small[PAIRS + crow] = at + 1
            small[PLIST + crow * (F * KP) + at] = pr
            for k in range(KD):
                w = cc[k * nc + c] - lowest
                sidx[pr * KD + k] = jnp.where((w >= 0) & (w < NW), i * NW + w, ZERO)
        return 0

    lax.fori_loop(0, F, pairs, 0)
    for n in range(LISTS):
        many = count[n]
        for u in range(2 * U - 1):
            row = (n * CAP + FRONT + many + u) * WORDS
            entries[row] = 0
            for k in range(KP):
                entries[row + 1 + k] = SPARE
        count[n] = (many + (2 * U - 1)) >> 3
    copies[-1].wait()


def planned(mine, their, p_cols, c_cols, a_tiles, p_tiles):
    mine, their = jnp.transpose(mine, (2, 1, 0)), jnp.transpose(their, (2, 1, 0))
    smem = lambda *shape: pltpu.SMEM(shape, jnp.int32)
    return call(
        plan_kernel,
        [("hbm", mine), ("vmem", their)] + [("hbm", x) for x in (p_cols.T, c_cols.T, a_tiles, p_tiles)],
        [
            ints(LISTS * CAP * WORDS),
            ints(8),
            ints(SMALL),
            ints(F * KP * KD),
            near((NA, T, T), jnp.bfloat16),
            near((5, F, KP, T, T), jnp.bfloat16),
            near((F * KP, T, T), jnp.bfloat16),
            near((NS, T, T), jnp.float32),
            near((NS, 2 * T, T), jnp.bfloat16),
        ],
        [
            smem(8),
            smem(*mine.shape),
            smem(*mine.shape),
            smem(p_cols.size),
            smem(c_cols.size // 2),
            pltpu.SemaphoreType.DMA((16,)),
        ],
    )


def entry_loop(n, count, entries, a, p, acc, sets):
    zero = jnp.zeros((T, T), jnp.bfloat16)

    def issue(low, high, at, u):
        word = entries[at + u * WORDS]
        tile = a[word & 255]
        j = word >> 8
        block, r = j >> 3, j & (F - 1)
        rhs = jnp.concatenate(
            [jnp.concatenate([p[block, r, 2 * k], p[block, r, 2 * k + 1]], axis=1) for k in range(2)], axis=0
        )
        pltpu.matmul_push_rhs(rhs, staging_register=(u // 2) % 2, mxu_index=u % 2)
        pltpu.matmul_acc_lhs(low[u], jnp.concatenate([tile, zero], axis=1), load_staged_rhs=(u // 2) % 2)
        pltpu.matmul_acc_lhs(high[u], jnp.concatenate([zero, tile], axis=1))

    def drain(low, high, at, u):
        for k, ref in enumerate((low[u], high[u])):
            x = pltpu.matmul_pop(ref)
            for e in range(2):
                slot = entries[at + u * WORDS + 1 + 2 * k + e]
                acc[slot] += x[:, e * T : (e + 1) * T]

    def double(t, _):
        at = (n * CAP + FRONT + 2 * U * t) * WORDS
        for u in range(U):
            issue(*sets[0], at, u)
            drain(*sets[1], at - U * WORDS, u)
        for u in range(U):
            issue(*sets[1], at + U * WORDS, u)
            drain(*sets[0], at, u)
        return 0

    many = count[n]
    lax.fori_loop(0, many, double, 0)
    for u in range(U):
        drain(*sets[1], (n * CAP + 2 * U * many) * WORDS, u)


def with_sets(work):
    def body(*refs):
        refs = list(refs)
        sets = []
        for _ in range(2):
            sets.append(([refs.pop(0) for _ in range(U)], [refs.pop(0) for _ in range(U)]))
        for low, high in sets:
            for ref in (*low, *high):
                pltpu.matmul_pop(ref)
        work(sets)

    pl.run_scoped(body, *[pltpu.ACC(u % 2)((T, 2 * T), jnp.float32) for _ in range(4) for u in range(U)])


OUTER, INNER, OWN = 0, C, 2 * C


def form_rows(first, quarters, coded, accs, small, sidx, sp, pt, out, *ex):
    for c in range(C):

        def pair(r, _):
            pr = small[PLIST + (first + c) * (F * KP) + r]
            tile = pt[pr]
            lhs = jnp.concatenate([tile, tile], axis=1)
            for n, acc in enumerate(accs):
                k = pr * KD + quarters[0] * KG + 2 * n
                rhs = jnp.concatenate([sp[sidx[k]], sp[sidx[k + 1]]], axis=1)
                pltpu.matmul_push_rhs(rhs, staging_register=(n // 2) % 2, mxu_index=n % 2)
                pltpu.matmul_acc_lhs(acc, lhs, load_staged_rhs=(n // 2) % 2)
            return 0

        lax.fori_loop(0, small[PAIRS + first + c], pair, 0)
        for n, acc in enumerate(accs):
            x = pltpu.matmul_pop(acc)
            for e in range(2):
                q, k = divmod(2 * n + e, KG)
                y = x[:, e * T : (e + 1) * T]
                if coded:
                    t = c * KG + k
                    out[q, t * T : (t + 1) * T, :] = code(y, ex[0].at[q], t)
                else:
                    out[c, k] = y
    if coded:
        for q in range(len(quarters)):
            out[q, ROWS:PACK, :] = ex[0][q].astype(jnp.int32).astype(jnp.int16)


def part_kernel(n, blocks, count, entries, *refs):
    new = refs[: len(blocks)]
    a, p, acc, _ = refs[-4:]
    for block, ref in zip(blocks, new):
        p[block] = ref[...]
    with_sets(lambda sets: entry_loop(n, count, entries, a, p, acc, sets))


def part(n, tabs, state, blocks):
    args = [("smem", x) for x in tabs] + [("vmem", x) for x in (*blocks.values(), *state)]
    first = len(args) - len(state)
    return call(
        functools.partial(part_kernel, n, tuple(blocks)),
        args,
        [near(x.shape, x.dtype) for x in state],
        alias={first + n: n for n in range(len(state))},
    )


def last_kernel(count, entries, small, sidx, their, pt, *refs):
    _, p, acc, sp, out, ex = refs[-6:]

    def halves(t, _):
        for u in range(4):
            n = t * 4 + u
            x = acc[n]
            hi = x.astype(jnp.bfloat16)
            sp[n, 0:T, :] = hi
            sp[n, T : 2 * T, :] = (x - hi.astype(jnp.float32)).astype(jnp.bfloat16)
        return 0

    def work(sets):
        entry_loop(LISTS - 1, count, entries, their, p, acc, sets)
        lax.fori_loop(0, F * NW // 4, halves, 0)
        form_rows(OWN, (0,), True, sets[0][0][:2], small, sidx, sp, pt, out, ex)

    with_sets(work)


def last(lists, tabs, state, their, pt):
    args = [("smem", x) for x in (*lists, *tabs)] + [("vmem", x) for x in (their, pt, *state)]
    first = len(args) - len(state)
    return call(
        last_kernel,
        args,
        [near(x.shape, x.dtype) for x in state] + [near((1, PACK, T), jnp.int16)],
        [pltpu.VMEM((1, SCALES, T), jnp.float32)],
        alias={first + n: n for n in range(len(state))},
    )[3:]


def coarse_kernel(first, quarters, coded, small, sidx, sp, pt, out, *ex):
    def body(*accs):
        for acc in accs:
            pltpu.matmul_pop(acc)
        form_rows(first, quarters, coded, accs, small, sidx, sp, pt, out, *ex)

    pl.run_scoped(body, *[pltpu.ACC(n % 2)((T, 2 * T), jnp.float32) for n in range(len(quarters) * KG // 2)])


def coarse(first, quarters, coded, tabs, sp, pt):
    n = len(quarters)
    out = near((n, PACK, T), jnp.int16) if coded else near((C, KG, T, T), jnp.float32)
    return call(
        functools.partial(coarse_kernel, first, quarters, coded),
        [("smem", tabs[0]), ("smem", tabs[1]), ("vmem", sp), ("vmem", pt)],
        [out],
        [pltpu.VMEM((n, SCALES, T), jnp.float32)] if coded else [],
    )[0]


def tiles():
    return [(c * KG + k, c, k, slice((c * KG + k) * T, (c * KG + k + 1) * T)) for c in range(C) for k in range(KG)]


def scale(ref, rows):
    ref[...] = jnp.exp2(widen(rows)) * (1.0 / LEVELS)


def add_kernel(own, *refs):
    *coded, out, ex = refs
    coded = [x.at[x.shape[0] - 1] for x in coded]
    for n, x in enumerate(coded):
        scale(ex.at[n], x[ROWS:PACK, :])
    for t, c, k, rows in tiles():
        y = own[c, k]
        for n, x in enumerate(coded):
            y = y + widen(x[rows, :]) * ex[n, t : t + 1, :]
        out[c, k] = y


def added(own, coded):
    return call(
        add_kernel,
        [("vmem", x) for x in (own, *coded)],
        [near(own.shape, own.dtype)],
        [pltpu.VMEM((len(coded), SCALES, T), jnp.float32)],
    )[0]


def finish_kernel(own, *refs):
    *coded, out_hbm, out, ex, sem = refs
    coded = [x.at[x.shape[0] - 1] for x in coded]
    for n, x in enumerate(coded):
        scale(ex.at[n], x[ROWS:PACK, :])
    copies = [pltpu.make_async_copy(out.at[c], out_hbm.at[c], sem.at[c]) for c in range(C)]
    for t, c, k, rows in tiles():
        y = own[c, k]
        for n, x in enumerate(coded):
            y = y + widen(x[rows, :]) * ex[n, t : t + 1, :]
        out[c, k] = y
        if k == KG - 1:
            copies[c].start()
    for copy in copies:
        copy.wait()


def finished(own, coded):
    return call(
        finish_kernel,
        [("vmem", x) for x in (own, *coded)],
        [("hbm", jax.ShapeDtypeStruct(own.shape, own.dtype))],
        [
            pltpu.VMEM(own.shape, own.dtype),
            pltpu.VMEM((len(coded), SCALES, T), jnp.float32),
            pltpu.SemaphoreType.DMA((C,)),
        ],
    )[0]


def along(x, to):
    n = lax.axis_size("row")
    return lax.ppermute(x, "row", [(i, to(i)) for i in range(n) if 0 <= to(i) < n])


def across(x, to, row=lambda r: r):
    rows, n = lax.axis_size("row"), lax.axis_size("grp")
    return lax.ppermute(
        x,
        ("grp", "row"),
        [
            (g * rows + r, to(g, r % 2) * rows + row(r))
            for r in range(rows)
            for g in range(n)
            if 0 <= row(r) < rows
        ],
    )


def partner(g, core):
    return g ^ (3 if core else 1)


def second(g, core):
    return partner(g, 1 - core)


def other(i):
    return i ^ 1


def away(i):
    return i - 1 if i % 2 == 0 else i + 1


def body(a_tiles, a_cols, p_tiles, p_cols, c_cols):
    tiles = a_tiles.reshape(NA, T, T)
    their_cols = across(a_cols, partner)
    their_tiles = across(tiles, partner)
    turn = along(p_tiles, lambda i: i - 2 if i % 2 == 0 else i + 2)
    beside = along(p_tiles, other)
    keep = along(p_tiles, lambda i: i + 2 if i % 2 == 0 else i - 2)
    entries, count, small, sidx, a, p, pt, acc, sp = planned(
        a_cols, their_cols, p_cols, c_cols, tiles, p_tiles
    )
    lists, state = (count, entries), (a, p, acc, sp)
    state = part(0, lists, state, {1: beside})
    far = along(turn, other)
    state = part(1, lists, state, {2: turn, 3: far})
    state = part(2, lists, state, {4: keep})
    sp, x = last(lists, (small, sidx), state, their_tiles, pt)
    rows = ((small, sidx), sp, pt)
    from_second = across(x, second)
    x = coarse(OUTER, (0,), True, *rows)
    from_skew = across(x, second, away)
    x = coarse(INNER, (0,), True, *rows)
    from_side = across(x, second, other)
    x = coarse(OUTER, (1,), True, *rows)
    outer = along(x, away)
    x = coarse(INNER, (1,), True, *rows)
    inner = along(x, other)
    own = coarse(OWN, (1,), False, *rows)
    mine = added(own, (from_second, from_side))
    return finished(mine, (from_skew, outer, inner))


def solution(mesh):
    return jax.shard_map(
        body,
        mesh=mesh,
        in_specs=(
            P("row", "grp", None, None, None),
            P("row", "grp", None),
            P("row", None, None, None),
            P(),
            P(),
        ),
        out_specs=P("row", "grp", None, None),
        check_vma=False,
    )
```

```python
import functools

import jax
import jax.numpy as jnp
from jax import lax
from jax.experimental import pallas as pl
from jax.experimental.pallas import tpu as pltpu
from jax.sharding import PartitionSpec as P


T = 128
F = 8
C = 4
S = 7
KP = 4
KC = 16
G = 4
KG = KC // G
KD = 2 * KG
NA = F * S
SCALES = C * KG
ROWS = SCALES * T
PACK = ROWS + SCALES
LEVELS = 32760.0
MB = 1 << 20

NW = 7 * C
SPARE = F * NW
ZERO = SPARE + 1
NS = ZERO + 1

LISTS = 4
U = 4
FRONT = U
CAP = FRONT + NA + 2 * U
WORDS = 1 + KP
PAIRS, PLIST = 0, 16
SMALL = PLIST + 3 * C * F * KP

SMEM = pl.BlockSpec(memory_space=pltpu.SMEM)
VMEM = pl.BlockSpec(memory_space=pltpu.VMEM)
HBM = pl.BlockSpec(memory_space=pltpu.HBM)


def call(kernel, args, outs, scratch=(), alias={}, mib=4):
    spec = {"smem": SMEM, "vmem": VMEM, "hbm": HBM}
    put = {
        "smem": lambda x: pltpu.with_memory_space_constraint(x, pltpu.SMEM),
        "vmem": lambda x: pltpu.with_memory_space_constraint(x, pltpu.VMEM),
        "hbm": lambda x: pltpu.with_memory_space_constraint(x, pltpu.HBM),
    }
    return pl.pallas_call(
        kernel,
        out_shape=[x for _, x in outs],
        in_specs=[spec[where] for where, _ in args],
        out_specs=[spec[where] for where, _ in outs],
        scratch_shapes=scratch,
        input_output_aliases=alias,
        compiler_params=pltpu.CompilerParams(vmem_limit_bytes=mib * MB),
        cost_estimate=pl.CostEstimate(flops=2 * 10**7, bytes_accessed=10**6, transcendentals=0),
    )(*(put[where](x) for where, x in args))


def ints(n):
    return ("smem", pltpu.SMEM((n,), jnp.int32))


def near(shape, dtype):
    return ("vmem", pltpu.VMEM(shape, dtype))


def code(x, scratch, row):
    top = jnp.maximum(jnp.max(jnp.abs(x), axis=0, keepdims=True), 1e-37)
    exponent = jnp.floor(jnp.log2(top)) + 1.0
    scratch[pl.ds(row, 1), :] = exponent
    return jnp.round(x * (jnp.exp2(-exponent) * LEVELS)).astype(jnp.int32).astype(jnp.int16)


def widen(x):
    return x.astype(jnp.int32).astype(jnp.float32)


def place_of(axis):
    return lax.axis_index(axis).astype(jnp.int32)


def started(sem, *pairs):
    copies = [pltpu.make_async_copy(src, dst, sem.at[n]) for n, (src, dst) in enumerate(pairs)]
    for c in copies:
        c.start()
    return copies


def plan_kernel(
    mine_hbm, their_vmem, pc_hbm, cc_hbm, tiles_hbm, p_hbm,
    entries, count, small, sidx, tiles, p, pt, acc,
    source, mine, their, pc, cc, sem,
):
    b, g = place_of("row"), place_of("grp")
    odd = lax.rem(b, 2)
    quarters = (jnp.where(odd == 0, 3 - g, g + 1 - 2 * (g & 1)) * KG, g * KG)
    np, nc = pc_hbm.shape[1], cc_hbm.shape[1]
    copies = started(
        sem,
        (mine_hbm, mine),
        (their_vmem, their),
        (p_hbm, p.at[0]),
        *((pc_hbm.at[k], pc.at[pl.ds(k * np, np)]) for k in range(KP)),
        *((cc_hbm.at[quarters[k // KG] + k % KG], cc.at[pl.ds(k * nc, nc)]) for k in range(KD)),
        (tiles_hbm, tiles),
    )
    for n in range(LISTS):
        count[n] = 0
        for u in range(FRONT):
            row = (n * CAP + u) * WORDS
            entries[row] = 0
            for k in range(KP):
                entries[row + 1 + k] = SPARE
    source[2] = 0
    source[1] = jnp.where(odd == 0, 3, 1)
    source[3] = jnp.where(odd == 0, 1, 3)
    source[0] = jnp.where(odd == 0, 4, 2)
    source[4] = jnp.where(odd == 0, 2, 4)
    for n in range(PLIST):
        small[n] = 0
    lowest = (b - 3) * C

    def clear(n, _):
        for w in range(4):
            acc[n * 4 + w] = jnp.zeros((T, T), jnp.float32)
        return 0

    lax.fori_loop(0, F * NW // 4, clear, 0)
    acc[ZERO] = jnp.zeros((T, T), jnp.float32)
    for c in copies[:-1]:
        c.wait()

    for which, cols in enumerate((mine, their)):

        def enter(i, _):
            for s in range(S):
                j = cols[s, 0, i]
                block = source[(j >> 3) - b + 2]
                n = 3 if which else block >> 1
                at = count[n]
                count[n] = at + 1
                row = (n * CAP + FRONT + at) * WORDS
                entries[row] = (i * S + s) | ((block * F + (j & (F - 1))) << 8)
                for k in range(KP):
                    entries[row + 1 + k] = pc[k * np + j] + (i * NW - lowest)
            return 0

        lax.fori_loop(0, F, enter, 0)

    def pairs(i, _):
        for q in range(KP):
            pr = i * KP + q
            pt[pr] = p[0, i, q].T
            c = pc[q * np + b * F + i]
            local = c - (b - 1) * C
            block = local >> 2
            kind = jnp.where(block == 1, 2, jnp.where((block == 0) == (odd == 0), 0, 1))
            crow = kind * C + (local & (C - 1))
            at = small[PAIRS + crow]
            small[PAIRS + crow] = at + 1
            small[PLIST + crow * (F * KP) + at] = pr
            for k in range(KD):
                w = cc[k * nc + c] - lowest
                sidx[pr * KD + k] = jnp.where((w >= 0) & (w < NW), i * NW + w, ZERO)
        return 0

    lax.fori_loop(0, F, pairs, 0)
    for n in range(LISTS):
        many = count[n]
        for u in range(2 * U - 1):
            row = (n * CAP + FRONT + many + u) * WORDS
            entries[row] = 0
            for k in range(KP):
                entries[row + 1 + k] = SPARE
        count[n] = (many + (2 * U - 1)) >> 3
    copies[-1].wait()


def planned(mine, their, p_cols, c_cols, a_tiles, p_tiles):
    mine, their = jnp.transpose(mine, (2, 1, 0)), jnp.transpose(their, (2, 1, 0))
    smem = lambda *shape: pltpu.SMEM(shape, jnp.int32)
    return call(
        plan_kernel,
        [("hbm", mine), ("vmem", their)] + [("hbm", x) for x in (p_cols.T, c_cols.T, a_tiles, p_tiles)],
        [
            ints(LISTS * CAP * WORDS),
            ints(8),
            ints(SMALL),
            ints(F * KP * KD),
            near((NA, T, T), jnp.bfloat16),
            near((5, F, KP, T, T), jnp.bfloat16),
            near((F * KP, T, T), jnp.bfloat16),
            near((NS, T, T), jnp.float32),
        ],
        [
            smem(8),
            smem(*mine.shape),
            smem(*mine.shape),
            smem(p_cols.size),
            smem(c_cols.size // 2),
            pltpu.SemaphoreType.DMA((16,)),
        ],
    )


def entry_loop(n, count, entries, a, p, acc, sets):
    zero = jnp.zeros((T, T), jnp.bfloat16)

    def issue(low, high, at, u):
        word = entries[at + u * WORDS]
        tile = a[word & 255]
        j = word >> 8
        block, r = j >> 3, j & (F - 1)
        rhs = jnp.concatenate(
            [jnp.concatenate([p[block, r, 2 * k], p[block, r, 2 * k + 1]], axis=1) for k in range(2)], axis=0
        )
        pltpu.matmul_push_rhs(rhs, staging_register=(u // 2) % 2, mxu_index=u % 2)
        pltpu.matmul_acc_lhs(low[u], jnp.concatenate([tile, zero], axis=1), load_staged_rhs=(u // 2) % 2)
        pltpu.matmul_acc_lhs(high[u], jnp.concatenate([zero, tile], axis=1))

    def drain(low, high, at, u):
        for k, ref in enumerate((low[u], high[u])):
            x = pltpu.matmul_pop(ref)
            for e in range(2):
                slot = entries[at + u * WORDS + 1 + 2 * k + e]
                acc[slot] += x[:, e * T : (e + 1) * T]

    def double(t, _):
        at = (n * CAP + FRONT + 2 * U * t) * WORDS
        for u in range(U):
            issue(*sets[0], at, u)
            drain(*sets[1], at - U * WORDS, u)
        for u in range(U):
            issue(*sets[1], at + U * WORDS, u)
            drain(*sets[0], at, u)
        return 0

    many = count[n]
    lax.fori_loop(0, many, double, 0)
    for u in range(U):
        drain(*sets[1], (n * CAP + 2 * U * many) * WORDS, u)


def with_sets(work):
    def body(*refs):
        refs = list(refs)
        sets = []
        for _ in range(2):
            sets.append(([refs.pop(0) for _ in range(U)], [refs.pop(0) for _ in range(U)]))
        for low, high in sets:
            for ref in (*low, *high):
                pltpu.matmul_pop(ref)
        work(sets)

    pl.run_scoped(body, *[pltpu.ACC(u % 2)((T, 2 * T), jnp.float32) for _ in range(4) for u in range(U)])


OUTER, INNER, OWN = 0, C, 2 * C


def terms(x):
    hi = x.astype(jnp.bfloat16)
    return jnp.concatenate([hi, (x - hi.astype(jnp.float32)).astype(jnp.bfloat16)], axis=0)


def form_rows(first, quarters, coded, accs, small, sidx, sums, pt, out, *ex):
    for c in range(C):

        def pair(r, _):
            pr = small[PLIST + (first + c) * (F * KP) + r]
            tile = pt[pr]
            lhs = jnp.concatenate([tile, tile], axis=1)
            for n, acc in enumerate(accs):
                k = pr * KD + quarters[0] * KG + 2 * n
                rhs = jnp.concatenate([terms(sums[sidx[k]]), terms(sums[sidx[k + 1]])], axis=1)
                pltpu.matmul_push_rhs(rhs, staging_register=(n // 2) % 2, mxu_index=n % 2)
                pltpu.matmul_acc_lhs(acc, lhs, load_staged_rhs=(n // 2) % 2)
            return 0

        lax.fori_loop(0, small[PAIRS + first + c], pair, 0)
        for n, acc in enumerate(accs):
            x = pltpu.matmul_pop(acc)
            for e in range(2):
                q, k = divmod(2 * n + e, KG)
                y = x[:, e * T : (e + 1) * T]
                if coded:
                    t = c * KG + k
                    out[q, t * T : (t + 1) * T, :] = code(y, ex[0].at[q], t)
                else:
                    out[c, k] = y
    if coded:
        for q in range(len(quarters)):
            out[q, ROWS:PACK, :] = ex[0][q].astype(jnp.int32).astype(jnp.int16)


def part_kernel(n, blocks, count, entries, *refs):
    new = refs[: len(blocks)]
    a, p, acc = refs[-3:]
    for block, ref in zip(blocks, new):
        p[block] = ref[...]
    with_sets(lambda sets: entry_loop(n, count, entries, a, p, acc, sets))


def part(n, tabs, state, blocks):
    args = [("smem", x) for x in tabs] + [("vmem", x) for x in (*blocks.values(), *state)]
    first = len(args) - len(state)
    return call(
        functools.partial(part_kernel, n, tuple(blocks)),
        args,
        [near(x.shape, x.dtype) for x in state],
        alias={first + n: n for n in range(len(state))},
    )


def last_kernel(count, entries, small, sidx, their, pt, *refs):
    _, p, acc, out, ex = refs[-5:]

    def work(sets):
        entry_loop(LISTS - 1, count, entries, their, p, acc, sets)
        form_rows(OWN, (0,), True, sets[0][0][:2], small, sidx, acc, pt, out, ex)

    with_sets(work)


def last(lists, tabs, state, their, pt):
    args = [("smem", x) for x in (*lists, *tabs)] + [("vmem", x) for x in (their, pt, *state)]
    first = len(args) - len(state)
    return call(
        last_kernel,
        args,
        [near(x.shape, x.dtype) for x in state] + [near((1, PACK, T), jnp.int16)],
        [pltpu.VMEM((1, SCALES, T), jnp.float32)],
        alias={first + n: n for n in range(len(state))},
    )[2:]


def coarse_kernel(first, quarters, coded, small, sidx, sums, pt, out, *ex):
    def body(*accs):
        for acc in accs:
            pltpu.matmul_pop(acc)
        form_rows(first, quarters, coded, accs, small, sidx, sums, pt, out, *ex)

    pl.run_scoped(body, *[pltpu.ACC(n % 2)((T, 2 * T), jnp.float32) for n in range(len(quarters) * KG // 2)])


def coarse(first, quarters, coded, tabs, sums, pt):
    n = len(quarters)
    out = near((n, PACK, T), jnp.int16) if coded else near((C, KG, T, T), jnp.float32)
    return call(
        functools.partial(coarse_kernel, first, quarters, coded),
        [("smem", tabs[0]), ("smem", tabs[1]), ("vmem", sums), ("vmem", pt)],
        [out],
        [pltpu.VMEM((n, SCALES, T), jnp.float32)] if coded else [],
    )[0]


def tiles():
    return [(c * KG + k, c, k, slice((c * KG + k) * T, (c * KG + k + 1) * T)) for c in range(C) for k in range(KG)]


def scale(ref, rows):
    ref[...] = jnp.exp2(widen(rows)) * (1.0 / LEVELS)


def add_kernel(own, *refs):
    *coded, out, ex = refs
    coded = [x.at[x.shape[0] - 1] for x in coded]
    for n, x in enumerate(coded):
        scale(ex.at[n], x[ROWS:PACK, :])
    for t, c, k, rows in tiles():
        y = own[c, k]
        for n, x in enumerate(coded):
            y = y + widen(x[rows, :]) * ex[n, t : t + 1, :]
        out[c, k] = y


def added(own, coded):
    return call(
        add_kernel,
        [("vmem", x) for x in (own, *coded)],
        [near(own.shape, own.dtype)],
        [pltpu.VMEM((len(coded), SCALES, T), jnp.float32)],
    )[0]


def finish_kernel(own, *refs):
    *coded, out_hbm, out, ex, sem = refs
    coded = [x.at[x.shape[0] - 1] for x in coded]
    for n, x in enumerate(coded):
        scale(ex.at[n], x[ROWS:PACK, :])
    copies = [pltpu.make_async_copy(out.at[c], out_hbm.at[c], sem.at[c]) for c in range(C)]
    for t, c, k, rows in tiles():
        y = own[c, k]
        for n, x in enumerate(coded):
            y = y + widen(x[rows, :]) * ex[n, t : t + 1, :]
        out[c, k] = y
        if k == KG - 1:
            copies[c].start()
    for copy in copies:
        copy.wait()


def finished(own, coded):
    return call(
        finish_kernel,
        [("vmem", x) for x in (own, *coded)],
        [("hbm", jax.ShapeDtypeStruct(own.shape, own.dtype))],
        [
            pltpu.VMEM(own.shape, own.dtype),
            pltpu.VMEM((len(coded), SCALES, T), jnp.float32),
            pltpu.SemaphoreType.DMA((C,)),
        ],
    )[0]


def along(x, to):
    n = lax.axis_size("row")
    return lax.ppermute(x, "row", [(i, to(i)) for i in range(n) if 0 <= to(i) < n])


def across(x, to, row=lambda r: r):
    rows, n = lax.axis_size("row"), lax.axis_size("grp")
    return lax.ppermute(
        x,
        ("grp", "row"),
        [
            (g * rows + r, to(g, r % 2) * rows + row(r))
            for r in range(rows)
            for g in range(n)
            if 0 <= row(r) < rows
        ],
    )


def partner(g, core):
    return g ^ (3 if core else 1)


def second(g, core):
    return partner(g, 1 - core)


def other(i):
    return i ^ 1


def away(i):
    return i - 1 if i % 2 == 0 else i + 1


def body(a_tiles, a_cols, p_tiles, p_cols, c_cols):
    tiles = a_tiles.reshape(NA, T, T)
    their_cols = across(a_cols, partner)
    their_tiles = across(tiles, partner)
    turn = along(p_tiles, lambda i: i - 2 if i % 2 == 0 else i + 2)
    beside = along(p_tiles, other)
    keep = along(p_tiles, lambda i: i + 2 if i % 2 == 0 else i - 2)
    entries, count, small, sidx, a, p, pt, acc = planned(
        a_cols, their_cols, p_cols, c_cols, tiles, p_tiles
    )
    lists, state = (count, entries), (a, p, acc)
    state = part(0, lists, state, {1: beside})
    far = along(turn, other)
    state = part(1, lists, state, {2: turn, 3: far})
    state = part(2, lists, state, {4: keep})
    sums, x = last(lists, (small, sidx), state, their_tiles, pt)
    rows = ((small, sidx), sums, pt)
    from_second = across(x, second)
    x = coarse(OUTER, (0,), True, *rows)
    from_skew = across(x, second, away)
    x = coarse(INNER, (0,), True, *rows)
    from_side = across(x, second, other)
    x = coarse(OUTER, (1,), True, *rows)
    outer = along(x, away)
    x = coarse(INNER, (1,), True, *rows)
    inner = along(x, other)
    own = coarse(OWN, (1,), False, *rows)
    mine = added(own, (from_second, from_side))
    return finished(mine, (from_skew, outer, inner))


def solution(mesh):
    return jax.shard_map(
        body,
        mesh=mesh,
        in_specs=(
            P("row", "grp", None, None, None),
            P("row", "grp", None),
            P("row", None, None, None),
            P(),
            P(),
        ),
        out_specs=P("row", "grp", None, None),
        check_vma=False,
    )
```

```python
import functools

import jax
import jax.numpy as jnp
from jax import lax
from jax.experimental import pallas as pl
from jax.experimental.pallas import tpu as pltpu
from jax.sharding import PartitionSpec as P


T = 128
F = 8
C = 4
S = 7
KP = 4
KC = 16
G = 4
KG = KC // G
KD = 2 * KG
NA = F * S
SCALES = C * KG
ROWS = SCALES * T
PACK = ROWS + SCALES
LEVELS = 32760.0
MB = 1 << 20

NW = 7 * C
SPARE = F * NW
ZERO = SPARE + 1
NS = ZERO + 1

LISTS = 4
U = 4
FRONT = U
CAP = FRONT + NA + 2 * U
WORDS = 1 + KP
PAIRS, PLIST = 0, 16
SMALL = PLIST + 3 * C * F * KP

SMEM = pl.BlockSpec(memory_space=pltpu.SMEM)
VMEM = pl.BlockSpec(memory_space=pltpu.VMEM)
HBM = pl.BlockSpec(memory_space=pltpu.HBM)


def call(kernel, args, outs, scratch=(), alias={}, mib=4):
    spec = {"smem": SMEM, "vmem": VMEM, "hbm": HBM}
    put = {
        "smem": lambda x: pltpu.with_memory_space_constraint(x, pltpu.SMEM),
        "vmem": lambda x: pltpu.with_memory_space_constraint(x, pltpu.VMEM),
        "hbm": lambda x: pltpu.with_memory_space_constraint(x, pltpu.HBM),
    }
    return pl.pallas_call(
        kernel,
        out_shape=[x for _, x in outs],
        in_specs=[spec[where] for where, _ in args],
        out_specs=[spec[where] for where, _ in outs],
        scratch_shapes=scratch,
        input_output_aliases=alias,
        compiler_params=pltpu.CompilerParams(vmem_limit_bytes=mib * MB),
        cost_estimate=pl.CostEstimate(flops=2 * 10**7, bytes_accessed=10**6, transcendentals=0),
    )(*(put[where](x) for where, x in args))


def ints(n):
    return ("smem", pltpu.SMEM((n,), jnp.int32))


def near(shape, dtype):
    return ("vmem", pltpu.VMEM(shape, dtype))


def code(x, scratch, row):
    top = jnp.maximum(jnp.max(jnp.abs(x), axis=0, keepdims=True), 1e-37)
    exponent = jnp.floor(jnp.log2(top)) + 1.0
    scratch[pl.ds(row, 1), :] = exponent
    return jnp.round(x * (jnp.exp2(-exponent) * LEVELS)).astype(jnp.int32).astype(jnp.int16)


def widen(x):
    return x.astype(jnp.int32).astype(jnp.float32)


def place_of(axis):
    return lax.axis_index(axis).astype(jnp.int32)


def started(sem, *pairs):
    copies = [pltpu.make_async_copy(src, dst, sem.at[n]) for n, (src, dst) in enumerate(pairs)]
    for c in copies:
        c.start()
    return copies


def plan_kernel(
    mine_hbm, their_vmem, pc_hbm, cc_hbm, tiles_hbm, p_hbm,
    entries, count, small, sidx, tiles, p, pt, acc,
    source, mine, their, pc, cc, sem,
):
    b, g = place_of("row"), place_of("grp")
    odd = lax.rem(b, 2)
    quarters = (jnp.where(odd == 0, 3 - g, g + 1 - 2 * (g & 1)) * KG, g * KG)
    np, nc = pc_hbm.shape[1], cc_hbm.shape[1]
    copies = started(
        sem,
        (mine_hbm, mine),
        (their_vmem, their),
        (p_hbm, p.at[0]),
        *((pc_hbm.at[k], pc.at[pl.ds(k * np, np)]) for k in range(KP)),
        *((cc_hbm.at[quarters[k // KG] + k % KG], cc.at[pl.ds(k * nc, nc)]) for k in range(KD)),
        (tiles_hbm, tiles),
    )
    for n in range(LISTS):
        count[n] = 0
        for u in range(FRONT):
            row = (n * CAP + u) * WORDS
            entries[row] = 0
            for k in range(KP):
                entries[row + 1 + k] = SPARE
    source[2] = 0
    source[1] = jnp.where(odd == 0, 3, 1)
    source[3] = jnp.where(odd == 0, 1, 3)
    source[0] = jnp.where(odd == 0, 4, 2)
    source[4] = jnp.where(odd == 0, 2, 4)
    for n in range(PLIST):
        small[n] = 0
    lowest = (b - 3) * C

    def clear(n, _):
        for w in range(4):
            acc[n * 4 + w] = jnp.zeros((T, T), jnp.float32)
        return 0

    lax.fori_loop(0, F * NW // 4, clear, 0)
    acc[ZERO] = jnp.zeros((T, T), jnp.float32)
    for c in copies[:-1]:
        c.wait()

    for which, cols in enumerate((mine, their)):

        def enter(i, _):
            for s in range(S):
                j = cols[s, 0, i]
                block = source[(j >> 3) - b + 2]
                n = 3 if which else block >> 1
                at = count[n]
                count[n] = at + 1
                row = (n * CAP + FRONT + at) * WORDS
                entries[row] = (i * S + s) | ((block * F + (j & (F - 1))) << 8)
                for k in range(KP):
                    entries[row + 1 + k] = pc[k * np + j] + (i * NW - lowest)
            return 0

        lax.fori_loop(0, F, enter, 0)

    def pairs(i, _):
        for q in range(KP):
            pr = i * KP + q
            pt[pr] = p[0, i, q].T
            c = pc[q * np + b * F + i]
            local = c - (b - 1) * C
            block = local >> 2
            kind = jnp.where(block == 1, 2, jnp.where((block == 0) == (odd == 0), 0, 1))
            crow = kind * C + (local & (C - 1))
            at = small[PAIRS + crow]
            small[PAIRS + crow] = at + 1
            small[PLIST + crow * (F * KP) + at] = pr
            for k in range(KD):
                w = cc[k * nc + c] - lowest
                sidx[pr * KD + k] = jnp.where((w >= 0) & (w < NW), i * NW + w, ZERO)
        return 0

    lax.fori_loop(0, F, pairs, 0)
    for n in range(LISTS):
        many = count[n]
        for u in range(2 * U - 1):
            row = (n * CAP + FRONT + many + u) * WORDS
            entries[row] = 0
            for k in range(KP):
                entries[row + 1 + k] = SPARE
        count[n] = (many + (2 * U - 1)) >> 3
    copies[-1].wait()


def planned(mine, their, p_cols, c_cols, a_tiles, p_tiles):
    mine, their = jnp.transpose(mine, (2, 1, 0)), jnp.transpose(their, (2, 1, 0))
    smem = lambda *shape: pltpu.SMEM(shape, jnp.int32)
    return call(
        plan_kernel,
        [("hbm", mine), ("vmem", their)] + [("hbm", x) for x in (p_cols.T, c_cols.T, a_tiles, p_tiles)],
        [
            ints(LISTS * CAP * WORDS),
            ints(8),
            ints(SMALL),
            ints(F * KP * KD),
            near((NA, T, T), jnp.bfloat16),
            near((5, F, KP, T, T), jnp.bfloat16),
            near((F * KP, T, T), jnp.bfloat16),
            near((NS, T, T), jnp.float32),
        ],
        [
            smem(8),
            smem(*mine.shape),
            smem(*mine.shape),
            smem(p_cols.size),
            smem(c_cols.size // 2),
            pltpu.SemaphoreType.DMA((16,)),
        ],
    )


def entry_loop(n, count, entries, a, p, acc, sets):
    zero = jnp.zeros((T, T), jnp.bfloat16)

    def issue(low, high, at, u):
        word = entries[at + u * WORDS]
        tile = a[word & 255]
        j = word >> 8
        block, r = j >> 3, j & (F - 1)
        rhs = jnp.concatenate(
            [jnp.concatenate([p[block, r, 2 * k], p[block, r, 2 * k + 1]], axis=1) for k in range(2)], axis=0
        )
        pltpu.matmul_push_rhs(rhs, staging_register=(u // 2) % 2, mxu_index=u % 2)
        pltpu.matmul_acc_lhs(low[u], jnp.concatenate([tile, zero], axis=1), load_staged_rhs=(u // 2) % 2)
        pltpu.matmul_acc_lhs(high[u], jnp.concatenate([zero, tile], axis=1))

    def drain(low, high, at, u):
        for k, ref in enumerate((low[u], high[u])):
            x = pltpu.matmul_pop(ref)
            for e in range(2):
                slot = entries[at + u * WORDS + 1 + 2 * k + e]
                acc[slot] += x[:, e * T : (e + 1) * T]

    def double(t, _):
        at = (n * CAP + FRONT + 2 * U * t) * WORDS
        for u in range(U):
            issue(*sets[0], at, u)
            drain(*sets[1], at - U * WORDS, u)
        for u in range(U):
            issue(*sets[1], at + U * WORDS, u)
            drain(*sets[0], at, u)
        return 0

    many = count[n]
    lax.fori_loop(0, many, double, 0)
    for u in range(U):
        drain(*sets[1], (n * CAP + 2 * U * many) * WORDS, u)


def with_sets(work):
    def body(*refs):
        refs = list(refs)
        sets = []
        for _ in range(2):
            sets.append(([refs.pop(0) for _ in range(U)], [refs.pop(0) for _ in range(U)]))
        for low, high in sets:
            for ref in (*low, *high):
                pltpu.matmul_pop(ref)
        work(sets)

    pl.run_scoped(body, *[pltpu.ACC(u % 2)((T, 2 * T), jnp.float32) for _ in range(4) for u in range(U)])


OUTER, INNER, OWN = 0, C, 2 * C


def terms(x):
    hi = x.astype(jnp.bfloat16)
    return jnp.concatenate([hi, (x - hi.astype(jnp.float32)).astype(jnp.bfloat16)], axis=0)


def form_rows(first, quarters, coded, sets, small, sidx, sums, pt, out, *ex, add=()):
    def take(c):
        for n, acc in enumerate(sets[c % 2]):
            x = pltpu.matmul_pop(acc)
            for e in range(2):
                q, k = divmod(2 * n + e, KG)
                y = x[:, e * T : (e + 1) * T]
                if coded:
                    t = c * KG + k
                    out[q, t * T : (t + 1) * T, :] = code(y, ex[0].at[q], t)
                else:
                    t = c * KG + k
                    for m, x_m in enumerate(add):
                        y = y + widen(x_m[t * T : (t + 1) * T, :]) * ex[0][m, t : t + 1, :]
                    out[c, k] = y

    for c in range(C):

        def pair(r, _):
            pr = small[PLIST + (first + c) * (F * KP) + r]
            tile = pt[pr]
            lhs = jnp.concatenate([tile, tile], axis=1)
            for n, acc in enumerate(sets[c % 2]):
                k = pr * KD + quarters[0] * KG + 2 * n
                rhs = jnp.concatenate([terms(sums[sidx[k]]), terms(sums[sidx[k + 1]])], axis=1)
                pltpu.matmul_push_rhs(rhs, staging_register=(n // 2) % 2, mxu_index=n % 2)
                pltpu.matmul_acc_lhs(acc, lhs, load_staged_rhs=(n // 2) % 2)
            return 0

        lax.fori_loop(0, small[PAIRS + first + c], pair, 0)
        if c:
            take(c - 1)
    take(C - 1)
    if coded:
        for q in range(len(quarters)):
            out[q, ROWS:PACK, :] = ex[0][q].astype(jnp.int32).astype(jnp.int16)


def part_kernel(n, blocks, count, entries, *refs):
    new = refs[: len(blocks)]
    a, p, acc = refs[-3:]
    for block, ref in zip(blocks, new):
        p[block] = ref[...]
    with_sets(lambda sets: entry_loop(n, count, entries, a, p, acc, sets))


def part(n, tabs, state, blocks):
    args = [("smem", x) for x in tabs] + [("vmem", x) for x in (*blocks.values(), *state)]
    first = len(args) - len(state)
    return call(
        functools.partial(part_kernel, n, tuple(blocks)),
        args,
        [near(x.shape, x.dtype) for x in state],
        alias={first + n: n for n in range(len(state))},
    )


def last_kernel(count, entries, small, sidx, their, pt, *refs):
    _, p, acc, out, ex = refs[-5:]

    def work(sets):
        entry_loop(LISTS - 1, count, entries, their, p, acc, sets)
        form_rows(OWN, (0,), True, [low[:2] for low, _ in sets], small, sidx, acc, pt, out, ex)

    with_sets(work)


def last(lists, tabs, state, their, pt):
    args = [("smem", x) for x in (*lists, *tabs)] + [("vmem", x) for x in (their, pt, *state)]
    first = len(args) - len(state)
    return call(
        last_kernel,
        args,
        [near(x.shape, x.dtype) for x in state] + [near((1, PACK, T), jnp.int16)],
        [pltpu.VMEM((1, SCALES, T), jnp.float32)],
        alias={first + n: n for n in range(len(state))},
    )[2:]


def coarse_kernel(first, quarters, coded, received, small, sidx, sums, pt, *refs):
    add, (out, *ex) = refs[:received], refs[received:]
    add = [x.at[x.shape[0] - 1] for x in add]
    for n, x in enumerate(add):
        scale(ex[0].at[n], x[ROWS:PACK, :])

    def body(*accs):
        for acc in accs:
            pltpu.matmul_pop(acc)
        many = len(accs) // 2
        form_rows(first, quarters, coded, (accs[:many], accs[many:]), small, sidx, sums, pt, out, *ex, add=add)

    many = len(quarters) * KG // 2
    pl.run_scoped(body, *[pltpu.ACC(n % 2)((T, 2 * T), jnp.float32) for _ in range(2) for n in range(many)])


def coarse(first, quarters, coded, tabs, sums, pt, received=()):
    n = len(quarters)
    out = near((n, PACK, T), jnp.int16) if coded else near((C, KG, T, T), jnp.float32)
    return call(
        functools.partial(coarse_kernel, first, quarters, coded, len(received)),
        [("smem", tabs[0]), ("smem", tabs[1])] + [("vmem", x) for x in (sums, pt, *received)],
        [out],
        [pltpu.VMEM((n if coded else len(received), SCALES, T), jnp.float32)],
    )[0]


def tiles():
    return [(c * KG + k, c, k, slice((c * KG + k) * T, (c * KG + k + 1) * T)) for c in range(C) for k in range(KG)]


def scale(ref, rows):
    ref[...] = jnp.exp2(widen(rows)) * (1.0 / LEVELS)


def finish_kernel(own, *refs):
    *coded, out_hbm, out, ex, sem = refs
    coded = [x.at[x.shape[0] - 1] for x in coded]
    for n, x in enumerate(coded):
        scale(ex.at[n], x[ROWS:PACK, :])
    copies = [pltpu.make_async_copy(out.at[c], out_hbm.at[c], sem.at[c]) for c in range(C)]
    for t, c, k, rows in tiles():
        y = own[c, k]
        for n, x in enumerate(coded):
            y = y + widen(x[rows, :]) * ex[n, t : t + 1, :]
        out[c, k] = y
        if k == KG - 1:
            copies[c].start()
    for copy in copies:
        copy.wait()


def finished(own, coded):
    return call(
        finish_kernel,
        [("vmem", x) for x in (own, *coded)],
        [("hbm", jax.ShapeDtypeStruct(own.shape, own.dtype))],
        [
            pltpu.VMEM(own.shape, own.dtype),
            pltpu.VMEM((len(coded), SCALES, T), jnp.float32),
            pltpu.SemaphoreType.DMA((C,)),
        ],
    )[0]


def along(x, to):
    n = lax.axis_size("row")
    return lax.ppermute(x, "row", [(i, to(i)) for i in range(n) if 0 <= to(i) < n])


def across(x, to, row=lambda r: r):
    rows, n = lax.axis_size("row"), lax.axis_size("grp")
    return lax.ppermute(
        x,
        ("grp", "row"),
        [
            (g * rows + r, to(g, r % 2) * rows + row(r))
            for r in range(rows)
            for g in range(n)
            if 0 <= row(r) < rows
        ],
    )


def partner(g, core):
    return g ^ (3 if core else 1)


def second(g, core):
    return partner(g, 1 - core)


def other(i):
    return i ^ 1


def away(i):
    return i - 1 if i % 2 == 0 else i + 1


def body(a_tiles, a_cols, p_tiles, p_cols, c_cols):
    tiles = a_tiles.reshape(NA, T, T)
    their_cols = across(a_cols, partner)
    their_tiles = across(tiles, partner)
    turn = along(p_tiles, lambda i: i - 2 if i % 2 == 0 else i + 2)
    beside = along(p_tiles, other)
    keep = along(p_tiles, lambda i: i + 2 if i % 2 == 0 else i - 2)
    entries, count, small, sidx, a, p, pt, acc = planned(
        a_cols, their_cols, p_cols, c_cols, tiles, p_tiles
    )
    lists, state = (count, entries), (a, p, acc)
    state = part(0, lists, state, {1: beside})
    far = along(turn, other)
    state = part(1, lists, state, {2: turn, 3: far})
    state = part(2, lists, state, {4: keep})
    sums, x = last(lists, (small, sidx), state, their_tiles, pt)
    rows = ((small, sidx), sums, pt)
    from_second = across(x, second)
    x = coarse(OUTER, (0,), True, *rows)
    from_skew = across(x, second, away)
    x = coarse(INNER, (0,), True, *rows)
    from_side = across(x, second, other)
    x = coarse(OUTER, (1,), True, *rows)
    outer = along(x, away)
    x = coarse(INNER, (1,), True, *rows)
    inner = along(x, other)
    own = coarse(OWN, (1,), False, *rows, (from_second, from_skew))
    return finished(own, (from_side, outer, inner))


def solution(mesh):
    return jax.shard_map(
        body,
        mesh=mesh,
        in_specs=(
            P("row", "grp", None, None, None),
            P("row", "grp", None),
            P("row", None, None, None),
            P(),
            P(),
        ),
        out_specs=P("row", "grp", None, None),
        check_vma=False,
    )
```
